256 devices in a mesh: row: 8 (over x, core), col: 32 (over y, z).
Axes of the slice: x: 4, y: 4, z: 8, core: 2. Of those that a mesh axis runs over, the one named last changes fastest.
Arguments:
- rhs: float32 [8, 32, 8, 4, 128], P('row', 'col'), may hold values from -6 to 6
- diag0: float32 [8, 32, 8, 128], P('row', 'col'), may hold values from 2 to 4
- blocks0: float32 [8, 32, 8, 14, 128, 128], P('row', 'col'), may hold values from -0.1875 to 0.1875
- cols0: int32 [8, 32, 8, 14], P('row', 'col'), may hold values from 0 to 23
- sends0: int32 [8, 32, 4, 4], P('row', 'col'), may hold values from 0 to 7
- pro0: float32 [8, 32, 8, 128, 128], P('row', 'col'), may hold values from -0.5 to 0.5
- agg0: int32 [8, 32, 8], P('row', 'col'), may hold values from 0 to 1
- diag1: float32 [8, 32, 2, 128], P('row', 'col'), may hold values from 2 to 4
- blocks1: float32 [8, 32, 2, 14, 128, 128], P('row', 'col'), may hold values from -0.1875 to 0.1875
- cols1: int32 [8, 32, 2, 14], P('row', 'col'), may hold values from 0 to 9
- sends1: int32 [8, 32, 4, 2], P('row', 'col'), may hold values from 0 to 1
- pro1: float32 [8, 32, 2, 128, 128], P('row', 'col'), may hold values from -0.25 to 0.25
- agg1: int32 [8, 32, 2], P('row', 'col'), may hold values from 0 to 63
- cinv: float32 [8192, 8192], P(('row', 'col')), may hold values from -0.0625 to 0.0625
Outputs:
- solution: float32 [8, 32, 8, 4, 128], P('row', 'col')
The draws below stay inside these ranges and needn't reach their ends.
Inputs may be any that keep to these rules, and one draw needn't show every extreme that they name: `sends0`: indices of the sender's own fine blocks. `sends1`: indices of the sender's own level-one blocks. `cols0`: indices into the extended fine vector of 24 blocks. `cols1`: indices into the extended level-one vector of 10 blocks. `agg0`: a level-one block of the same partition. `agg1`: a coarsest block, on any partition.
All inputs are finite; a program needn't handle non-finite values.
Results may differ from the reference program's by a relative error of at most 0.0001.
Values sent between devices are 32-bit elements; how exact they have to be, the bound alone decides.
A program may use at most 64 MiB of HBM per device.

```python
import math
import jax
import jax.numpy as jnp
from jax import lax

BS = 128
NB = 8
NB1 = 2
K = 14
K1 = 14
G0 = 4
G1 = 2
NRHS = 4
NU = 2
NCB = 64
NCU = 8192
N_ROW = 8
N_COL = 32


def touch_ends(result, key, least, top_value):
    place = [jax.random.randint(jax.random.fold_in(key, axis), (), 0, length) for axis, length in enumerate(result.shape)]
    longest = result.shape.index(max(result.shape))
    next_to = place[:longest] + [(place[longest] + 1) % result.shape[longest]] + place[longest + 1:]
    return result.at[tuple(place)].set(least).at[tuple(next_to)].set(top_value)


def steps_of(stream_key, shape, shards, least, largest):
    gain = 1.0
    for dim, blocks in shards:
        steps = jax.random.uniform(jax.random.fold_in(jax.random.fold_in(stream_key, 6), dim), (blocks,), jnp.float32, least / len(shards), largest / len(shards))
        gain = gain * jnp.repeat(jnp.exp(steps), shape[dim] // blocks).reshape((-1,) + (1,) * (len(shape) - 1 - dim))
    return gain


def bell_draw(key, shape, spread, most, cuts=(), dtype=jnp.bfloat16):
    drawn = jax.random.normal(key, shape, jnp.float32) * spread
    if len(cuts) > 0:
        drawn = steps_of(key, shape, cuts, -0.22, 0.18) * drawn
    return jnp.clip(drawn, min=-most, max=most).astype(dtype)


def setup_inputs(seed: int = 0) -> dict:
    splits = jax.random.split(jax.random.key(seed), 15)
    rhs = bell_draw(splits[0], (N_ROW, N_COL, NB, NRHS, BS), 1.0, 6.0, ((0, 8), (1, 32)), jnp.float32)
    diag0 = jnp.clip(jnp.exp(math.log(4.0) - 0.6931472 * jax.random.uniform(splits[1], (N_ROW, N_COL, NB, BS), jnp.float32) ** steps_of(splits[1], (N_ROW, N_COL, NB, BS), ((0, 8), (1, 32)), -0.2, 0.2)), 2.0, 4.0)
    blocks0 = bell_draw(splits[2], (N_ROW, N_COL, NB, K, BS, BS), (K * BS // 2) ** -0.5, 0.1875, ((0, 8), (1, 32)), jnp.float32)
    cols0 = touch_ends(jax.random.randint(splits[3], (N_ROW, N_COL, NB, K), 0, NB + 4 * G0), jax.random.fold_in(splits[3], 1), 0, (NB + 4 * G0) - 1).astype(jnp.int32)
    sends0 = touch_ends(jax.random.randint(splits[4], (N_ROW, N_COL, 4, G0), 0, NB), jax.random.fold_in(splits[4], 1), 0, NB - 1).astype(jnp.int32)
    pro0 = bell_draw(splits[5], (N_ROW, N_COL, NB, BS, BS), BS ** -0.5, 0.5, ((0, 8), (1, 32)), jnp.float32)
    agg0 = touch_ends(jax.random.randint(splits[6], (N_ROW, N_COL, NB), 0, NB1), jax.random.fold_in(splits[6], 1), 0, NB1 - 1).astype(jnp.int32)
    diag1 = jnp.clip(jnp.exp(math.log(4.0) - 0.6931472 * jax.random.uniform(splits[7], (N_ROW, N_COL, NB1, BS), jnp.float32) ** steps_of(splits[7], (N_ROW, N_COL, NB1, BS), ((0, 8), (1, 32)), -0.2, 0.2)), 2.0, 4.0)
    blocks1 = bell_draw(splits[8], (N_ROW, N_COL, NB1, K1, BS, BS), (K1 * BS // 2) ** -0.5, 0.1875, ((0, 8), (1, 32)), jnp.float32)
    cols1 = touch_ends(jax.random.randint(splits[9], (N_ROW, N_COL, NB1, K1), 0, NB1 + 4 * G1), jax.random.fold_in(splits[9], 1), 0, (NB1 + 4 * G1) - 1).astype(jnp.int32)
    sends1 = touch_ends(jax.random.randint(splits[10], (N_ROW, N_COL, 4, G1), 0, NB1), jax.random.fold_in(splits[10], 1), 0, NB1 - 1).astype(jnp.int32)
    pro1 = bell_draw(splits[11], (N_ROW, N_COL, NB1, BS, BS), (4 * BS) ** -0.5, 0.25, ((0, 8), (1, 32)), jnp.float32)
    agg1 = touch_ends(jax.random.randint(splits[12], (N_ROW, N_COL, NB1), 0, NCB), jax.random.fold_in(splits[12], 1), 0, NCB - 1).astype(jnp.int32)
    cinv = bell_draw(splits[13], (NCU, NCU), NCU ** -0.5, 0.0625, ((0, 256),), jnp.float32)
    return dict(rhs=rhs, diag0=diag0, blocks0=blocks0, cols0=cols0, sends0=sends0, pro0=pro0, agg0=agg0, diag1=diag1, blocks1=blocks1, cols1=cols1, sends1=sends1, pro1=pro1, agg1=agg1, cinv=cinv)


HIGH = lax.Precision.HIGHEST
OMEGA = 0.3


def gather_ghosts(vector, sends):
    packed = jax.vmap(jax.vmap(lambda blocks, picks: blocks[picks]))(vector, sends)
    zero_row = jnp.zeros_like(packed[:1, :, 0])
    zero_col = jnp.zeros_like(packed[:, :1, 0])
    above = jnp.concatenate([zero_row, packed[:-1, :, 0]], axis=0)
    below = jnp.concatenate([packed[1:, :, 1], zero_row], axis=0)
    left = jnp.concatenate([zero_col, packed[:, :-1, 2]], axis=1)
    right = jnp.concatenate([packed[:, 1:, 3], zero_col], axis=1)
    return jnp.concatenate([vector, above, below, left, right], axis=2)


def apply_op(vector, diag, blocks, cols, sends):
    extended = gather_ghosts(vector, sends)
    nearby = jax.vmap(jax.vmap(lambda source, picks: source[picks]))(extended, cols)
    coupled = jnp.einsum('xybkij,xybkrj->xybri', blocks, nearby, precision=HIGH)
    return diag[..., None, :] * vector + coupled


def smooth(vector, right_side, diag, blocks, cols, sends, count):
    for sweep in range(count):
        vector = vector + OMEGA * (right_side - apply_op(vector, diag, blocks, cols, sends)) / diag[..., None, :]
    return vector


def reference(rhs, diag0, blocks0, cols0, sends0, pro0, agg0, diag1, blocks1, cols1, sends1, pro1, agg1, cinv):
    fine_x = OMEGA * rhs / diag0[..., None, :]
    fine_x = smooth(fine_x, rhs, diag0, blocks0, cols0, sends0, NU - 1)
    fine_res = rhs - apply_op(fine_x, diag0, blocks0, cols0, sends0)
    onehot0 = (agg0[..., None] == jnp.arange(NB1)).astype(jnp.float32)
    restricted = jnp.einsum('xybij,xybri->xybrj', pro0, fine_res, precision=HIGH)
    level_rhs = jnp.einsum('xybc,xybrj->xycrj', onehot0, restricted, precision=HIGH)
    level_x = OMEGA * level_rhs / diag1[..., None, :]
    level_x = smooth(level_x, level_rhs, diag1, blocks1, cols1, sends1, NU - 1)
    level_res = level_rhs - apply_op(level_x, diag1, blocks1, cols1, sends1)
    onehot1 = (agg1[..., None] == jnp.arange(NCB)).astype(jnp.float32)
    contrib = jnp.einsum('xybij,xybri->xybrj', pro1, level_res, precision=HIGH)
    coarse_rhs = jnp.einsum('xybc,xybrj->rcj', onehot1, contrib, precision=HIGH).reshape(NRHS, NCU)
    coarse_x = jnp.einsum('ij,rj->ri', cinv, coarse_rhs, precision=HIGH)
    coarse_blocks = coarse_x.reshape(NRHS, NCB, BS)
    picked = jnp.einsum('xybc,rcj->xybrj', onehot1, coarse_blocks, precision=HIGH)
    level_x = level_x + jnp.einsum('xybij,xybrj->xybri', pro1, picked, precision=HIGH)
    level_x = smooth(level_x, level_rhs, diag1, blocks1, cols1, sends1, NU)
    lifted = jnp.einsum('xybc,xycrj->xybrj', onehot0, level_x, precision=HIGH)
    fine_x = fine_x + jnp.einsum('xybij,xybrj->xybri', pro0, lifted, precision=HIGH)
    fine_x = smooth(fine_x, rhs, diag0, blocks0, cols0, sends0, NU)
    return fine_x
```

```python
import jax
import jax.numpy as jnp
from jax import lax
from jax.experimental import pallas as pl
from jax.experimental.pallas import tpu as pltpu
from jax.sharding import Mesh
from jax.sharding import PartitionSpec as P

OMEGA = 0.3
NX, NC, NY, NZ = 4, 2, 4, 8
BS = 128
NB, NB1, K, G0, G1, R = 8, 2, 14, 4, 2, 4
F32, BF16 = jnp.float32, jnp.bfloat16
MESH = pl.DeviceIdType.MESH
NT = (((1,), (1,)), ((), ()))
NN = (((1,), (0,)), ((), ()))


def split(v):
    hi = v.astype(BF16)
    lo = (v - hi.astype(F32)).astype(BF16)
    return hi, lo


def halves(v):
    hi = v.astype(BF16).astype(F32)
    return hi, v - hi


def eight(v):
    hi, lo = halves(v)
    return jnp.concatenate([hi, lo], axis=0).astype(BF16)


def fold(out):
    n = out.shape[1] // 2
    return (out[0:4, :n] + out[0:4, n:]) + (out[4:8, :n] + out[4:8, n:])


def dot(a, b, dims):
    return lax.dot_general(a, b, dims, preferred_element_type=F32)


def kernel(
    cols0, sends0, agg0, cols1, sends1, agg1,
    rhs, diag0, diag1, blocks0, pro0, blocks1, pro1, cinv,
    out,
    land0, land_p0, land1, land_p1, cin,
    w0, p0, w1, p1,
    ext0, ext1, x0, r0, x1, b1, pack0, ghost0, pack1, ghost1,
    osend, oz, oy, ot, dsend, dz, dy, xsend, xg, crhs, ez, ey, ef,
    lsem, gs, gr, ozs, ozr, oys, oyr, dzs, dzr, dys, dyr, xs, xr, ezs, ezr, eys, eyr, efs, efr, cs, cr,
    unroll,
):
    x, c, y, z = (lax.axis_index(a) for a in ("x", "c", "y", "z"))
    row = x * NC + c
    col = y * NZ + z
    loads = []

    def load(i, src, dst):
        copy = pltpu.make_async_copy(src, dst, lsem.at[i])
        copy.start()
        loads.append(copy)

    for b in range(NB):
        load(b, blocks0.at[0, 0, b], land0.at[b])
    load(NB, pro0.at[0, 0], land_p0)
    load(NB + 1, blocks1.at[0, 0], land1)
    load(NB + 2, pro1.at[0, 0], land_p1)
    load(NB + 3, cinv, cin.at[c])

    def by_row(r):
        r = lax.rem(r + 8, 8)
        return (lax.div(r, 2), lax.rem(r, 2), y, z)

    def by_col(q):
        q = lax.rem(q + 32, 32)
        return (x, c, lax.div(q, NZ), lax.rem(q, NZ))

    near = [by_row(row + 1), by_row(row - 1), by_col(col + 1), by_col(col - 1)]
    valid = [row > 0, row < 7, col > 0, col < 31]
    me_zc = z * 2 + c
    me_xc = row

    def zc_peer(k):
        t = lax.rem(me_zc + k, 16)
        return (x, lax.rem(t, 2), y, lax.div(t, 2))

    def z_peer(k):
        return (x, c, y, lax.rem(z + k, NZ))

    def y_peer(k):
        return (x, c, lax.rem(y + k, NY), z)

    def x_peer(k):
        return (lax.rem(x + k, NX), c, y, z)

    def xc_peer(k):
        t = lax.rem(me_xc + k, 8)
        return (lax.div(t, 2), lax.rem(t, 2), y, z)

    barrier = pltpu.get_barrier_semaphore()
    peers = near + [zc_peer(k) for k in range(1, 16)] + [y_peer(k) for k in range(1, 4)] + [xc_peer(k) for k in range(1, 8)]
    for peer in peers:
        pl.semaphore_signal(barrier, inc=1, device_id=peer, device_id_type=MESH)

    sent = []

    def send(src, dst, ssem, rsem, peer):
        copy = pltpu.make_async_remote_copy(
            src_ref=src, dst_ref=dst, send_sem=ssem, recv_sem=rsem, device_id=peer, device_id_type=MESH
        )
        copy.start()
        sent.append(copy)

    def arrive(dst, ssem, rsem):
        pltpu.make_async_remote_copy(
            src_ref=dst, dst_ref=dst, send_sem=ssem, recv_sem=rsem, device_id=(x, c, y, z), device_id_type=MESH
        ).wait_recv()

    def start_exchange(e, value, sends, pack, ghost, width, base):
        for d in range(4):
            for g in range(width):
                pack[e, d, g] = value[sends[d * width + g]]
        for d in range(4):
            send(pack.at[e, d], ghost.at[e, d], gs.at[base + e, d], gr.at[base + e, d], near[d])

    def own_part(value, ext, count):
        for b in range(count):
            hi, lo = halves(value[b])
            ext[b, 0:4] = hi
            ext[b, 4:8] = lo

    def end_exchange(e, ghost, ext, width, base, count):
        for d in range(4):
            arrive(ghost.at[e, d], gs.at[base + e, d], gr.at[base + e, d])
            for g in range(width):
                hi, lo = halves(jnp.where(valid[d], ghost[e, d, g], 0.0))
                ext[count + d * width + g, 0:4] = hi
                ext[count + d * width + g, 4:8] = lo

    def coupled(b, ext, cols, w):
        v = jnp.concatenate([ext[cols[b * K + k]] for k in range(K)], axis=1).astype(BF16)
        return fold(dot(v, w[b], NT))

    def each(count, body):
        if unroll >= count:
            for b in range(count):
                body(b)
        else:
            def step(t, carry):
                for u in range(unroll):
                    body(t * unroll + u)
                return carry
            lax.fori_loop(0, count // unroll, step, 0)

    def sweep(right, diag, value, ext, cols, w, count):
        def body(b):
            d = diag[b]
            v = value[b]
            value[b] = v + OMEGA * (right[b] - (d * v + coupled(b, ext, cols, w))) / d
        each(count, body)

    def residual(right, diag, value, ext, cols, w, count, res):
        def body(b):
            res[b] = right[b] - (diag[b] * value[b] + coupled(b, ext, cols, w))
        each(count, body)

    class First:
        def __init__(self, ref, vector):
            self.ref, self.vector = ref, vector

        def __getitem__(self, b):
            return self.ref[0, 0, pl.ds(b, 1), :] if self.vector else self.ref[0, 0, b]

    f0, d0, d1 = First(rhs, False), First(diag0, True), First(diag1, True)

    def level0(e):
        start_exchange(e, x0, sends0, pack0, ghost0, G0, 0)

    def level0_end(e):
        own_part(x0, ext0, NB)
        end_exchange(e, ghost0, ext0, G0, 0, NB)

    def level1(e):
        start_exchange(e, x1, sends1, pack1, ghost1, G1, 4)

    def level1_end(e):
        own_part(x1, ext1, NB1)
        end_exchange(e, ghost1, ext1, G1, 4, NB1)

    for b in range(NB):
        x0[b] = OMEGA * f0[b] / d0[b]
    pl.semaphore_wait(barrier, len(peers))
    level0(0)

    lanes = lax.broadcasted_iota(jnp.int32, (2, BS), 1)
    osend[0:2, :] = jnp.where(lanes == agg1[0], 1.0, 0.0)
    osend[2:4, :] = jnp.where(lanes == agg1[1], 1.0, 0.0)
    oz[me_zc] = osend[...]
    for k in (8, 7, 9, 6, 10, 5, 11, 4, 12, 3, 13, 2, 14, 1, 15):
        send(osend, oz.at[me_zc], ozs.at[k], ozr.at[me_zc], zc_peer(k))

    def split0(b, carry):
        pltpu.make_async_copy(blocks0.at[0, 0, b], land0.at[b], lsem.at[b]).wait()
        for k in range(K):
            hi, lo = split(land0[b, k])
            w0[b, 0:BS, k * BS:(k + 1) * BS] = hi
            w0[b, BS:2 * BS, k * BS:(k + 1) * BS] = lo
        return carry

    lax.fori_loop(0, NB, split0, 0)

    level0_end(0)
    sweep(f0, d0, x0, ext0, cols0, w0, NB)
    level0(1)
    own_part(x0, ext0, NB)

    loads[NB].wait()
    for b in range(NB):
        hi, lo = split(land_p0[b])
        p0[b * BS:(b + 1) * BS, 0:BS] = hi
        p0[b * BS:(b + 1) * BS, BS:2 * BS] = lo
    loads[NB + 3].wait()
    send(cin.at[c], cin.at[c], cs, cr, (x, 1 - c, y, z))
    for k in range(1, 16):
        t = lax.rem(me_zc + k, 16)
        arrive(oz.at[t], ozs.at[k], ozr.at[t])
    oy[y] = oz[...]
    for k in (2, 1, 3):
        send(oz, oy.at[y], oys.at[k], oyr.at[y], y_peer(k))

    end_exchange(1, ghost0, ext0, G0, 0, NB)
    residual(f0, d0, x0, ext0, cols0, w0, NB, r0)
    parts = [[], []]
    for b in range(NB):
        both = jnp.concatenate(halves(r0[b]), axis=0)
        for level in range(NB1):
            parts[level].append(jnp.where(agg0[b] == level, both, 0.0))
    lhs = jnp.concatenate([jnp.concatenate(p, axis=1) for p in parts], axis=0).astype(BF16)
    low = dot(lhs, p0[...], NN)
    for level in range(NB1):
        b1[level] = fold(low[level * 8:level * 8 + 8])
        x1[level] = OMEGA * b1[level] / d1[level]
    level1(0)

    loads[NB + 1].wait()
    for b in range(NB1):
        for k in range(K):
            hi, lo = split(land1[b, k])
            w1[b, 0:BS, k * BS:(k + 1) * BS] = hi
            w1[b, BS:2 * BS, k * BS:(k + 1) * BS] = lo
    loads[NB + 2].wait()
    for b in range(NB1):
        hi, lo = split(land_p1[b])
        p1[b, :, 0:BS] = hi
        p1[b, :, BS:2 * BS] = lo
    level1_end(0)
    sweep(b1, d1, x1, ext1, cols1, w1, NB1)
    level1(1)
    own_part(x1, ext1, NB1)

    for k in range(1, 4):
        t = lax.rem(y + k, NY)
        arrive(oy.at[t], oys.at[k], oyr.at[t])
    rows = []
    for q in range(NY):
        for t in range(8):
            rows.append(jnp.concatenate([oy[q, 2 * t], oy[q, 2 * t + 1]], axis=0))
    ot[...] = jnp.concatenate(rows, axis=0).T.astype(BF16)

    end_exchange(1, ghost1, ext1, G1, 4, NB1)
    for b in range(NB1):
        r1 = b1[b] - (d1[b] * x1[b] + coupled(b, ext1, cols1, w1))
        con = fold(dot(eight(r1), p1[b], NN))
        dsend[0, b * 2:b * 2 + 2, :] = con[0:2]
        dsend[1, b * 2:b * 2 + 2, :] = con[2:4]
    dz[me_zc] = dsend[c]
    for k in (8, 7, 9, 6, 10, 5, 11, 4, 12, 3, 13, 2, 14, 1, 15):
        peer = zc_peer(k)
        send(dsend.at[peer[1]], dz.at[me_zc], dzs.at[k], dzr.at[me_zc], peer)
    arrive(cin.at[1 - c], cs, cr)
    for k in range(1, 16):
        t = lax.rem(me_zc + k, 16)
        arrive(dz.at[t], dzs.at[k], dzr.at[t])
    dy[y] = dz[...]
    for k in (2, 1, 3):
        send(dz, dy.at[y], dys.at[k], dyr.at[y], y_peer(k))
    for k in range(1, 4):
        t = lax.rem(y + k, NY)
        arrive(dy.at[t], dys.at[k], dyr.at[t])
    rows = []
    for q in range(NY):
        for t in range(8):
            rows.append(jnp.concatenate([dy[q, 2 * t], dy[q, 2 * t + 1]], axis=0))
    got = jnp.concatenate(rows, axis=0)
    odd = lax.rem(lax.broadcasted_iota(jnp.int32, got.shape, 0), 2)
    ghi, glo = halves(got)
    rhs4 = jnp.concatenate(
        [jnp.where(odd == 0, ghi, 0.0), jnp.where(odd == 1, ghi, 0.0), jnp.where(odd == 0, glo, 0.0), jnp.where(odd == 1, glo, 0.0)],
        axis=1,
    ).astype(BF16)
    dense = dot(ot[...], rhs4, NN)
    xsend[...] = dense[0:64, 0:256] + dense[0:64, 256:512]
    for k in (2, 1, 3):
        send(xsend, xg.at[x], xs.at[k], xr.at[x], x_peer(k))
    total = xsend[...]
    for k in range(1, 4):
        t = lax.rem(x + k, NX)
        arrive(xg.at[t], xs.at[k], xr.at[t])
        total = total + xg[t]
    crhs[0] = total[:, 0:BS]
    crhs[1] = total[:, BS:2 * BS]

    def mat(t, acc):
        acc = list(acc)
        vec = [crhs[r, pl.ds(t, 1), :] for r in range(2)]
        for g in range(2):
            for m in range(4):
                a = cin[g, m * 8:m * 8 + 8, pl.ds(pl.multiple_of(t * BS, BS), BS)]
                for r in range(2):
                    acc[(g * 2 + r) * 4 + m] = acc[(g * 2 + r) * 4 + m] + a * vec[r]
        return tuple(acc)

    acc = lax.fori_loop(0, 64, mat, tuple(jnp.zeros((8, BS), F32) for _ in range(16)), unroll=4)
    zl = lax.rem(z, 4)
    chunks = []
    for q in range(4):
        for part in halves(jnp.concatenate(acc[q * 4:q * 4 + 4], axis=0)):
            chunks.append(jnp.concatenate([jnp.where(zl == s, part, 0.0) for s in range(4)], axis=0))
    place = jnp.concatenate(chunks, axis=1).astype(BF16)
    lhs_row = lax.broadcasted_iota(jnp.int32, (8, 8 * BS), 0)
    lhs_col = lax.div(lax.broadcasted_iota(jnp.int32, (8, 8 * BS), 1), 2 * BS)
    ones = jnp.where(lhs_row == lhs_col, 1.0, 0.0).astype(BF16)
    ez[z] = dot(ones, place, NT)[0:4]
    for k in (4, 3, 5, 2, 6, 1, 7):
        send(ez.at[z], ez.at[z], ezs.at[k], ezr.at[z], z_peer(k))
    for k in range(1, NZ):
        t = lax.rem(z + k, NZ)
        arrive(ez.at[t], ezs.at[k], ezr.at[t])
    for h in range(2):
        ey[y, h] = (ez[4 * h] + ez[4 * h + 1]) + (ez[4 * h + 2] + ez[4 * h + 3])
    for k in (2, 1, 3):
        send(ey.at[y], ey.at[y], eys.at[k], eyr.at[y], y_peer(k))
    for k in range(1, 4):
        t = lax.rem(y + k, NY)
        arrive(ey.at[t], eys.at[k], eyr.at[t])
    for q in range(NY):
        for h in range(2):
            ef[me_xc, q * 2 + h] = ey[q, h]
    for k in (4, 5, 3, 2, 6, 7, 1):
        send(ef.at[me_xc], ef.at[me_xc], efs.at[k], efr.at[me_xc], xc_peer(k))
    for k in range(1, 8):
        t = lax.rem(me_xc + k, 8)
        arrive(ef.at[t], efs.at[k], efr.at[t])
    for b in range(NB1):
        a = agg1[b]
        ax, ag, ayz = lax.div(a, 16), lax.rem(lax.div(a, 8), 2), lax.rem(a, 8)
        half = [ef[ax * 2 + core, ayz] for core in range(2)]
        pick = jnp.concatenate([jnp.where(ag == 0, h[0:2], h[2:4]) for h in half], axis=0)
        e8 = eight(pick)
        o = dot(jnp.concatenate([e8, e8], axis=1), p1[b], NT)
        x1[b] = x1[b] + (o[0:4] + o[4:8])

    for e in (2, 3):
        level1(e)
        level1_end(e)
        sweep(b1, d1, x1, ext1, cols1, w1, NB1)

    for b in range(NB):
        e8 = eight(x1[agg0[b]])
        o = dot(jnp.concatenate([e8, e8], axis=1), p0[b * BS:(b + 1) * BS, :], NT)
        x0[b] = x0[b] + (o[0:4] + o[4:8])
    for e in (2, 3):
        level0(e)
        level0_end(e)
        sweep(f0, d0, x0, ext0, cols0, w0, NB)
    for b in range(NB):
        out[0, 0, b] = x0[b]
    for copy in sent:
        copy.wait_send()


def on_device(rhs, diag0, blocks0, cols0, sends0, pro0, agg0, diag1, blocks1, cols1, sends1, pro1, agg1, cinv, unroll=8):
    vmem = pl.BlockSpec(memory_space=pltpu.VMEM)
    smem = pl.BlockSpec(memory_space=pltpu.SMEM)
    hbm = pl.BlockSpec(memory_space=pl.ANY)
    V = pltpu.VMEM
    dma = pltpu.SemaphoreType.DMA
    scratch = [
        V((NB, K, BS, BS), F32), V((NB, BS, BS), F32), V((NB1, K, BS, BS), F32), V((NB1, BS, BS), F32), V((2, 32, 8192), F32),
        V((NB, 2 * BS, K * BS), BF16), V((NB * BS, 2 * BS), BF16), V((NB1, 2 * BS, K * BS), BF16), V((NB1, BS, 2 * BS), BF16),
        V((NB + 4 * G0, 8, BS), F32), V((NB1 + 4 * G1, 8, BS), F32),
        V((NB, R, BS), F32), V((NB, R, BS), F32), V((NB1, R, BS), F32), V((NB1, R, BS), F32),
        V((4, 4, G0, R, BS), F32), V((4, 4, G0, R, BS), F32), V((4, 4, G1, R, BS), F32), V((4, 4, G1, R, BS), F32),
        V((4, BS), F32), V((16, 4, BS), F32), V((4, 16, 4, BS), F32), V((BS, 256), BF16),
        V((2, 4, BS), F32), V((16, 4, BS), F32), V((4, 16, 4, BS), F32),
        V((64, 256), F32), V((4, 64, 256), F32), V((2, 64, BS), F32),
        V((8, 4, BS), F32), V((4, 2, 4, BS), F32), V((8, 8, 4, BS), F32),
        dma((NB + 4,)), dma((8, 4)), dma((8, 4)),
        dma((16,)), dma((16,)), dma((4,)), dma((4,)),
        dma((16,)), dma((16,)), dma((4,)), dma((4,)),
        dma((4,)), dma((4,)), dma((8,)), dma((8,)), dma((4,)), dma((4,)), dma((8,)), dma((8,)),
        dma, dma,
    ]

    def body(*refs):
        kernel(*refs, unroll=unroll)

    return pl.pallas_call(
        body,
        out_shape=jax.ShapeDtypeStruct(rhs.shape, F32),
        in_specs=[smem] * 6 + [vmem] * 3 + [hbm] * 5,
        out_specs=vmem,
        scratch_shapes=scratch,
        compiler_params=pltpu.CompilerParams(collective_id=0, has_side_effects=True, vmem_limit_bytes=60 * 1024 * 1024),
        name="vcycle",
    )(
        cols0.reshape(-1), sends0.reshape(-1), agg0.reshape(-1), cols1.reshape(-1), sends1.reshape(-1), agg1.reshape(-1),
        rhs, diag0, diag1, blocks0, pro0, blocks1, pro1, cinv,
    )


def solution(mesh):
    finer = Mesh(mesh.devices.reshape(NX, NC, NY, NZ), ("x", "c", "y", "z"))
    ROW, COL = ("x", "c"), ("y", "z")
    ranks = (3, 2, 4, 2, 2, 3, 1, 2, 4, 2, 2, 3, 1)
    in_specs = tuple(P(ROW, COL, *([None] * n)) for n in ranks) + (P(ROW + COL, None),)
    return jax.shard_map(
        on_device, mesh=finer, in_specs=in_specs, out_specs=P(ROW, COL, None, None, None), check_vma=False
    )
```

```python
import jax
import jax.numpy as jnp
from jax import lax
from jax.experimental import pallas as pl
from jax.experimental.pallas import tpu as pltpu
from jax.sharding import Mesh
from jax.sharding import PartitionSpec as P

OMEGA = 0.3
NX, NC, NY, NZ = 4, 2, 4, 8
BS = 128
NB, NB1, K, G0, G1, R = 8, 2, 14, 4, 2, 4
F32, BF16 = jnp.float32, jnp.bfloat16
MESH = pl.DeviceIdType.MESH
NT = (((1,), (1,)), ((), ()))
NN = (((1,), (0,)), ((), ()))


def split(v):
    hi = v.astype(BF16)
    lo = (v - hi.astype(F32)).astype(BF16)
    return hi, lo


def turned(v):
    return jnp.concatenate(split(v.T), axis=1)


def halves(v):
    hi = v.astype(BF16).astype(F32)
    return hi, v - hi


def eight(v):
    hi, lo = halves(v)
    return jnp.concatenate([hi, lo], axis=0).astype(BF16)


def fold(out):
    n = out.shape[1] // 2
    return (out[0:4, :n] + out[0:4, n:]) + (out[4:8, :n] + out[4:8, n:])


def dot(a, b, dims):
    return lax.dot_general(a, b, dims, preferred_element_type=F32)


def kernel(
    cols0, sends0, agg0, cols1, sends1, agg1,
    rhs, diag0, diag1, blocks0, pro0, blocks1, pro1, cinv,
    out,
    rhs_v, diag0_v, diag1_v,
    land0, land_p0, land1, land_p1, cin,
    w0, p0, w1, p1, sel, pp1, gp1, ps1, gsel,
    ext0, ext1, x0, r0, x1, b1, pack0, ghost0, pack1, ghost1,
    osend, oz, oy, ot, dsend, dz, dy, xsend, xg, crhs, ez, ef,
    lsem, gs, gr, ozs, ozr, oys, oyr, dzs, dzr, dys, dyr, xs, xr, ezs, ezr, efs, efr, cs, cr,
    unroll,
):
    x, c, y, z = (lax.axis_index(a) for a in ("x", "c", "y", "z"))
    row = x * NC + c
    col = y * NZ + z
    loads = {}

    def load(i, src, dst):
        copy = pltpu.make_async_copy(src, dst, lsem.at[i])
        copy.start()
        loads[i] = copy

    def by_row(r):
        r = lax.rem(r + 8, 8)
        return (lax.div(r, 2), lax.rem(r, 2), y, z)

    def by_col(q):
        q = lax.rem(q + 32, 32)
        return (x, c, lax.div(q, NZ), lax.rem(q, NZ))

    near = [by_row(row + 1), by_row(row - 1), by_col(col + 1), by_col(col - 1)]
    valid = [row > 0, row < 7, col > 0, col < 31]
    me_zc = z * 2 + c

    def zc_peer(k):
        t = lax.rem(me_zc + k, 16)
        return (x, lax.rem(t, 2), y, lax.div(t, 2))

    def y_peer(k):
        return (x, c, lax.rem(y + k, NY), z)

    def x_peer(k):
        return (lax.rem(x + k, NX), c, y, z)

    me_xy = x * NY + y

    def xy_peer(k):
        return (lax.rem(x + k // 4, NX), c, lax.rem(y + k % 4, NY), z)

    barrier = pltpu.get_barrier_semaphore()
    peers = near + [zc_peer(k) for k in range(1, 16)] + [xy_peer(k) for k in range(1, 16)]
    for peer in peers:
        pl.semaphore_signal(barrier, inc=1, device_id=peer, device_id_type=MESH)

    load(NB + 4, rhs.at[0, 0], rhs_v)
    load(NB + 5, diag0.at[0, 0], diag0_v)
    load(NB + 6, diag1.at[0, 0], diag1_v)
    load(NB + 2, pro1.at[0, 0], land_p1)
    for b in range(NB):
        load(b, blocks0.at[0, 0, b], land0.at[b])
    load(NB, pro0.at[0, 0], land_p0)
    load(NB + 1, blocks1.at[0, 0], land1)
    load(NB + 3, cinv, cin.at[c])
    sent, due = [], {}

    def post(key, src, dst, ssem, rsem, peer, landing, landed):
        copy = pltpu.make_async_remote_copy(
            src_ref=src, dst_ref=dst, send_sem=ssem, recv_sem=rsem, device_id=peer, device_id_type=MESH
        )
        copy.start()
        sent.append(copy)
        due[key] = pltpu.make_async_remote_copy(
            src_ref=landing, dst_ref=landing, send_sem=ssem, recv_sem=landed, device_id=peer, device_id_type=MESH
        )

    def take(*key):
        due.pop(key).wait_recv()


    def start_exchange(e, value, pick, pack, ghost, width, base):
        for d in range(4):
            for g in range(width):
                pack[e, d, g] = value[pick(d, g)]
        for d in range(4):
            sems = gs.at[base + e, d], gr.at[base + e, d]
            post((base + e, d), pack.at[e, d], ghost.at[e, d], *sems, near[d], ghost.at[e, d], sems[1])

    def own_part(value, ext, count):
        for b in range(count):
            hi, lo = halves(value[b])
            ext[b, 0:4] = hi
            ext[b, 4:8] = lo

    def end_exchange(e, ghost, ext, width, base, count):
        for d in range(4):
            take(base + e, d)
            for g in range(width):
                hi, lo = halves(jnp.where(valid[d], ghost[e, d, g], 0.0))
                ext[count + d * width + g, 0:4] = hi
                ext[count + d * width + g, 4:8] = lo

    def coupled(b, ext, cols, w):
        v = jnp.concatenate([ext[cols[0, 0, b, k]] for k in range(K)], axis=1).astype(BF16)
        return fold(dot(v, w[b], NN))

    def each(count, body):
        if unroll >= count:
            for b in range(count):
                body(b)
        else:
            def step(t, carry):
                for u in range(unroll):
                    body(t * unroll + u)
                return carry
            lax.fori_loop(0, count // unroll, step, 0)

    def sweep(right, diag, value, ext, cols, w, count):
        def body(b):
            d = diag[b]
            v = value[b]
            value[b] = v + OMEGA * (right[b] - (d * v + coupled(b, ext, cols, w))) / d
        each(count, body)

    def residual(right, diag, value, ext, cols, w, count, res):
        def body(b):
            res[b] = right[b] - (diag[b] * value[b] + coupled(b, ext, cols, w))
        each(count, body)

    class First:
        def __init__(self, ref, vector):
            self.ref, self.vector = ref, vector

        def __getitem__(self, b):
            return self.ref[pl.ds(b, 1), :] if self.vector else self.ref[b]

    f0, d0, d1 = rhs_v, First(diag0_v, True), First(diag1_v, True)

    def level0(e):
        start_exchange(e, x0, lambda d, g: sends0[0, 0, d, g], pack0, ghost0, G0, 0)

    def level0_end(e):
        own_part(x0, ext0, NB)
        end_exchange(e, ghost0, ext0, G0, 0, NB)

    def level1(e):
        start_exchange(e, x1, lambda d, g: sends1[0, 0, g, d], pack1, ghost1, G1, 4)

    def level1_end(e):
        own_part(x1, ext1, NB1)
        end_exchange(e, ghost1, ext1, G1, 4, NB1)

    for n in (4, 5, 6):
        loads.pop(NB + n).wait()
    for b in range(NB):
        x0[b] = OMEGA * f0[b] / d0[b]
    pl.semaphore_wait(barrier, len(peers))
    level0(0)

    loads.pop(NB + 2).wait()
    spot = lax.broadcasted_iota(jnp.int32, (4, 256), 1)
    rr = lax.broadcasted_iota(jnp.int32, (4, 256), 0)

    def rows_of(a):
        ax, ag, ay, ah = lax.div(a, 16), lax.rem(lax.div(a, 8), 2), lax.rem(lax.div(a, 2), 4), lax.rem(a, 2)
        base = (ax * 4 + ay) * 16 + ah * 4 + ag * 2
        return jnp.where(spot == base + lax.div(rr, 2) * 8 + lax.rem(rr, 2), 1.0, 0.0)

    for d in range(4):
        for g in range(G1):
            pp1[d, g] = land_p1[sends1[0, 0, g, d]]
            ps1[d, g] = rows_of(agg1[0, 0, sends1[0, 0, g, d]])
    for d in range(4):
        post(("pp", d), pp1.at[d], gp1.at[d], gs.at[8, d], gr.at[8, d], near[d], gp1.at[d], gr.at[8, d])
        post(("ps", d), ps1.at[d], gsel.at[d], gs.at[9, d], gr.at[9, d], near[d], gsel.at[d], gr.at[9, d])
    lanes = lax.broadcasted_iota(jnp.int32, (2, BS), 1)
    osend[0:2, :] = jnp.where(lanes == agg1[0, 0, 0], 1.0, 0.0)
    osend[2:4, :] = jnp.where(lanes == agg1[0, 0, 1], 1.0, 0.0)
    oz[me_zc] = osend[...]
    for k in (8, 7, 9, 6, 10, 5, 11, 4, 12, 3, 13, 2, 14, 1, 15):
        t = lax.rem(me_zc + k, 16)
        post(("oz", k), osend, oz.at[me_zc], ozs.at[k], ozr.at[me_zc], zc_peer(k), oz.at[t], ozr.at[t])

    def split0(b, carry):
        pltpu.make_async_copy(blocks0.at[0, 0, b], land0.at[b], lsem.at[b]).wait()
        for k in range(K):
            w0[b, k * BS:(k + 1) * BS, :] = turned(land0[b, k])
        return carry

    lax.fori_loop(0, NB, split0, 0)
    for b in range(NB):
        loads.pop(b)

    level0_end(0)
    sweep(f0, d0, x0, ext0, cols0, w0, NB)
    level0(1)
    own_part(x0, ext0, NB)

    loads.pop(NB).wait()
    for b in range(NB):
        hi, lo = split(land_p0[b])
        p0[b * BS:(b + 1) * BS, 0:BS] = hi
        p0[b * BS:(b + 1) * BS, BS:2 * BS] = lo
    loads.pop(NB + 3).wait()
    post(("cin",), cin.at[c], cin.at[c], cs, cr, (x, 1 - c, y, z), cin.at[1 - c], cr)
    for k in range(1, 16):
        take("oz", k)
    oy[y] = oz[...]
    for k in (2, 1, 3):
        t = lax.rem(y + k, NY)
        post(("oy", k), oz, oy.at[y], oys.at[k], oyr.at[y], y_peer(k), oy.at[t], oyr.at[t])

    end_exchange(1, ghost0, ext0, G0, 0, NB)
    residual(f0, d0, x0, ext0, cols0, w0, NB, r0)
    parts = [[], []]
    for b in range(NB):
        both = jnp.concatenate(halves(r0[b]), axis=0)
        for level in range(NB1):
            parts[level].append(jnp.where(agg0[0, 0, b] == level, both, 0.0))
    lhs = jnp.concatenate([jnp.concatenate(p, axis=1) for p in parts], axis=0).astype(BF16)
    low = dot(lhs, p0[...], NN)
    for level in range(NB1):
        b1[level] = fold(low[level * 8:level * 8 + 8])
        x1[level] = OMEGA * b1[level] / d1[level]
    level1(0)

    loads.pop(NB + 1).wait()
    for b in range(NB1):
        for k in range(K):
            w1[b, k * BS:(k + 1) * BS, :] = turned(land1[b, k])
    for b in range(NB1):
        hi, lo = split(land_p1[b])
        p1[b, :, 0:BS] = hi
        p1[b, :, BS:2 * BS] = lo
        sel[b * 4:b * 4 + 4, :] = rows_of(agg1[0, 0, b]).astype(BF16)
    for d in range(4):
        take("pp", d)
        take("ps", d)
        for g in range(G1):
            n = NB1 + d * G1 + g
            hi, lo = split(gp1[d, g])
            p1[n, :, 0:BS] = hi
            p1[n, :, BS:2 * BS] = lo
            sel[n * 4:n * 4 + 4, :] = jnp.where(valid[d], gsel[d, g], 0.0).astype(BF16)
    level1_end(0)
    sweep(b1, d1, x1, ext1, cols1, w1, NB1)
    level1(1)
    own_part(x1, ext1, NB1)

    for k in range(1, 4):
        take("oy", k)
    rows = []
    for q in range(NY):
        for t in range(8):
            rows.append(jnp.concatenate([oy[q, 2 * t], oy[q, 2 * t + 1]], axis=0))
    ot[...] = jnp.concatenate(rows, axis=0).T.astype(BF16)

    end_exchange(1, ghost1, ext1, G1, 4, NB1)
    for b in range(NB1):
        r1 = b1[b] - (d1[b] * x1[b] + coupled(b, ext1, cols1, w1))
        con = fold(dot(eight(r1), p1[b], NN))
        dsend[0, b * 2:b * 2 + 2, :] = con[0:2]
        dsend[1, b * 2:b * 2 + 2, :] = con[2:4]
    dz[me_zc] = dsend[c]
    for k in (8, 7, 9, 6, 10, 5, 11, 4, 12, 3, 13, 2, 14, 1, 15):
        peer = zc_peer(k)
        t = lax.rem(me_zc + k, 16)
        post(("dz", k), dsend.at[peer[1]], dz.at[me_zc], dzs.at[k], dzr.at[me_zc], peer, dz.at[t], dzr.at[t])
    take("cin")
    for k in range(1, 16):
        take("dz", k)
    dy[y] = dz[...]
    for k in (2, 1, 3):
        t = lax.rem(y + k, NY)
        post(("dy", k), dz, dy.at[y], dys.at[k], dyr.at[y], y_peer(k), dy.at[t], dyr.at[t])
    for k in range(1, 4):
        take("dy", k)
    rows = []
    for q in range(NY):
        for t in range(8):
            rows.append(jnp.concatenate([dy[q, 2 * t], dy[q, 2 * t + 1]], axis=0))
    got = jnp.concatenate(rows, axis=0)
    odd = lax.rem(lax.broadcasted_iota(jnp.int32, got.shape, 0), 2)
    ghi, glo = halves(got)
    rhs4 = jnp.concatenate(
        [jnp.where(odd == 0, ghi, 0.0), jnp.where(odd == 1, ghi, 0.0), jnp.where(odd == 0, glo, 0.0), jnp.where(odd == 1, glo, 0.0)],
        axis=1,
    ).astype(BF16)
    dense = dot(ot[...], rhs4, NN)
    xsend[...] = dense[0:64, 0:256] + dense[0:64, 256:512]
    for k in (2, 1, 3):
        t = lax.rem(x + k, NX)
        post(("x", k), xsend, xg.at[x], xs.at[k], xr.at[x], x_peer(k), xg.at[t], xr.at[t])
    total = xsend[...]
    for k in range(1, 4):
        t = lax.rem(x + k, NX)
        take("x", k)
        total = total + xg[t]
    crhs[0] = total[:, 0:BS]
    crhs[1] = total[:, BS:2 * BS]

    def mat(t, acc):
        acc = list(acc)
        vec = [crhs[r, pl.ds(t, 1), :] for r in range(2)]
        for g in range(2):
            for m in range(4):
                a = cin[g, m * 8:m * 8 + 8, pl.ds(pl.multiple_of(t * BS, BS), BS)]
                for r in range(2):
                    acc[(g * 2 + r) * 4 + m] = acc[(g * 2 + r) * 4 + m] + a * vec[r]
        return tuple(acc)

    acc = lax.fori_loop(0, 64, mat, tuple(jnp.zeros((8, BS), F32) for _ in range(16)), unroll=4)
    zl = lax.rem(z, 4)
    chunks = []
    for q in range(4):
        for part in halves(jnp.concatenate(acc[q * 4:q * 4 + 4], axis=0)):
            chunks.append(jnp.concatenate([jnp.where(zl == s, part, 0.0) for s in range(4)], axis=0))
    place = jnp.concatenate(chunks, axis=1).astype(BF16)
    lhs_row = lax.broadcasted_iota(jnp.int32, (8, 8 * BS), 0)
    lhs_col = lax.div(lax.broadcasted_iota(jnp.int32, (8, 8 * BS), 1), 2 * BS)
    ones = jnp.where(lhs_row == lhs_col, 1.0, 0.0).astype(BF16)
    ez[me_zc] = dot(ones, place, NT)[0:4]
    for k in (8, 7, 9, 6, 10, 5, 11, 4, 12, 3, 13, 2, 14, 1, 15):
        t = lax.rem(me_zc + k, 16)
        post(("ez", k), ez.at[me_zc], ez.at[me_zc], ezs.at[k], ezr.at[me_zc], zc_peer(k), ez.at[t], ezr.at[t])
    for k in range(1, 16):
        take("ez", k)
    for h in range(2):
        for core in range(2):
            n = [ez[(4 * h + q) * 2 + core] for q in range(4)]
            ef[me_xy, core * 2 + h] = (n[0] + n[1]) + (n[2] + n[3])
    for k in (10, 9, 11, 6, 14, 2, 8, 5, 7, 13, 15, 1, 3, 4, 12):
        t = xy_peer(k)
        n = t[0] * NY + t[2]
        post(("ef", k), ef.at[me_xy], ef.at[me_xy], efs.at[k], efr.at[me_xy], t, ef.at[n], efr.at[n])
    for k in range(1, 16):
        take("ef", k)
    every = jnp.concatenate(
        [jnp.concatenate([ef[n, 2 * m], ef[n, 2 * m + 1]], axis=0) for n in range(16) for m in range(2)], axis=0
    )
    both = dot(sel[...], jnp.concatenate(split(every), axis=1), NN)
    picked = both[:, 0:BS] + both[:, BS:2 * BS]
    for n in range(NB1 + 4 * G1):
        e8 = eight(picked[n * 4:n * 4 + 4])
        o = dot(jnp.concatenate([e8, e8], axis=1), p1[n], NT)
        o = o[0:4] + o[4:8]
        if n < NB1:
            x1[n] = x1[n] + o
        else:
            hi, lo = halves(ext1[n, 0:4] + ext1[n, 4:8] + o)
            ext1[n, 0:4] = hi
            ext1[n, 4:8] = lo
    own_part(x1, ext1, NB1)
    for e in (2, 3):
        if e == 3:
            level1(e)
            level1_end(e)
        sweep(b1, d1, x1, ext1, cols1, w1, NB1)

    for b in range(NB):
        e8 = eight(x1[agg0[0, 0, b]])
        o = dot(jnp.concatenate([e8, e8], axis=1), p0[b * BS:(b + 1) * BS, :], NT)
        x0[b] = x0[b] + (o[0:4] + o[4:8])
    for e in (2, 3):
        level0(e)
        level0_end(e)
        sweep(f0, d0, x0, ext0, cols0, w0, NB)
    for b in range(NB):
        out[0, 0, b] = x0[b]
    for copy in sent:
        copy.wait_send()


def on_device(rhs, diag0, blocks0, cols0, sends0, pro0, agg0, diag1, blocks1, cols1, sends1, pro1, agg1, cinv, unroll=8):
    vmem = pl.BlockSpec(memory_space=pltpu.VMEM)
    smem = pl.BlockSpec(memory_space=pltpu.SMEM)
    hbm = pl.BlockSpec(memory_space=pl.ANY)
    V = pltpu.VMEM
    dma = pltpu.SemaphoreType.DMA
    scratch = [
        V((NB, R, BS), F32), V((NB, BS), F32), V((NB1, BS), F32),
        V((NB, K, BS, BS), F32), V((NB, BS, BS), F32), V((NB1, K, BS, BS), F32), V((NB1, BS, BS), F32), V((2, 32, 8192), F32),
        V((NB, K * BS, 2 * BS), BF16), V((NB * BS, 2 * BS), BF16), V((NB1, K * BS, 2 * BS), BF16), V((NB1 + 4 * G1, BS, 2 * BS), BF16), V((40, 256), BF16),
        V((4, G1, BS, BS), F32), V((4, G1, BS, BS), F32), V((4, G1, 4, 256), F32), V((4, G1, 4, 256), F32),
        V((NB + 4 * G0, 8, BS), F32), V((NB1 + 4 * G1, 8, BS), F32),
        V((NB, R, BS), F32), V((NB, R, BS), F32), V((NB1, R, BS), F32), V((NB1, R, BS), F32),
        V((4, 4, G0, R, BS), F32), V((4, 4, G0, R, BS), F32), V((4, 4, G1, R, BS), F32), V((4, 4, G1, R, BS), F32),
        V((4, BS), F32), V((16, 4, BS), F32), V((4, 16, 4, BS), F32), V((BS, 256), BF16),
        V((2, 4, BS), F32), V((16, 4, BS), F32), V((4, 16, 4, BS), F32),
        V((64, 256), F32), V((4, 64, 256), F32), V((2, 64, BS), F32),
        V((16, 4, BS), F32), V((16, 4, 4, BS), F32),
        dma((NB + 7,)), dma((10, 4)), dma((10, 4)),
        dma((16,)), dma((16,)), dma((4,)), dma((4,)),
        dma((16,)), dma((16,)), dma((4,)), dma((4,)),
        dma((4,)), dma((4,)), dma((16,)), dma((16,)), dma((16,)), dma((16,)),
        dma, dma,
    ]

    def body(*refs):
        kernel(*refs, unroll=unroll)

    return pl.pallas_call(
        body,
        out_shape=jax.ShapeDtypeStruct(rhs.shape, F32),
        in_specs=[smem] * 6 + [hbm] * 8,
        out_specs=vmem,
        scratch_shapes=scratch,
        compiler_params=pltpu.CompilerParams(collective_id=0, has_side_effects=True, vmem_limit_bytes=60 * 1024 * 1024),
        name="vcycle",
    )(
        cols0, sends0, agg0, cols1, sends1.transpose(0, 1, 3, 2), agg1,
        rhs, diag0, diag1, blocks0, pro0, blocks1, pro1, cinv,
    )


def solution(mesh):
    finer = Mesh(mesh.devices.reshape(NX, NC, NY, NZ), ("x", "c", "y", "z"))
    ROW, COL = ("x", "c"), ("y", "z")
    ranks = (3, 2, 4, 2, 2, 3, 1, 2, 4, 2, 2, 3, 1)
    in_specs = tuple(P(ROW, COL, *([None] * n)) for n in ranks) + (P(ROW + COL, None),)
    return jax.shard_map(
        on_device, mesh=finer, in_specs=in_specs, out_specs=P(ROW, COL, None, None, None), check_vma=False
    )
```

```python
import jax
import jax.numpy as jnp
from jax import lax
from jax.experimental import pallas as pl
from jax.experimental.pallas import tpu as pltpu
from jax.sharding import Mesh
from jax.sharding import PartitionSpec as P

OMEGA = 0.3
NX, NC, NY, NZ = 4, 2, 4, 8
BS = 128
NB, NB1, K, G0, G1, R = 8, 2, 14, 4, 2, 4
F32, BF16 = jnp.float32, jnp.bfloat16
MESH = pl.DeviceIdType.MESH
NT = (((1,), (1,)), ((), ()))
NN = (((1,), (0,)), ((), ()))


def split(v):
    hi = v.astype(BF16)
    lo = (v - hi.astype(F32)).astype(BF16)
    return hi, lo


def turned(eye, left, right):
    both = [jnp.concatenate(pair, axis=1) for pair in zip(split(left), split(right))]
    return dot(eye, jnp.concatenate(both, axis=0), NT).astype(BF16)


def halves(v):
    hi = v.astype(BF16).astype(F32)
    return hi, v - hi


def eight(v):
    hi, lo = halves(v)
    return jnp.concatenate([hi, lo], axis=0).astype(BF16)


def fold(out):
    n = out.shape[1] // 2
    return (out[0:4, :n] + out[0:4, n:]) + (out[4:8, :n] + out[4:8, n:])


def dot(a, b, dims):
    return lax.dot_general(a, b, dims, preferred_element_type=F32)


def kernel(
    cols0_h, sends0_h, agg0_h, cols1_h, sends1_h, agg1_h,
    rhs, diag0, diag1, blocks0, pro0, blocks1, pro1, cinv,
    out,
    cols0, sends0, agg0, cols1, sends1, agg1,
    rhs_v, diag0_v, diag1_v,
    land0, land_p0, land1, land_p1, cin,
    w0, p0, w1, p1, sel, pp1, gp1, ps1, gsel,
    ext0, ext1, x0, r0, x1, b1, pack0, ghost0, pack1, ghost1,
    osend, oz, oy, ot, dsend, dz, dy, xsend, xg, crhs, ez, ef,
    lsem, gs, gr, ozs, ozr, oys, oyr, dzs, dzr, dys, dyr, xs, xr, ezs, ezr, efs, efr, cs, cr,
    unroll,
):
    x, c, y, z = (lax.axis_index(a) for a in ("x", "c", "y", "z"))
    row = x * NC + c
    col = y * NZ + z
    loads = {}

    def load(i, src, dst):
        copy = pltpu.make_async_copy(src, dst, lsem.at[i])
        copy.start()
        loads[i] = copy

    def by_row(r):
        r = lax.rem(r + 8, 8)
        return (lax.div(r, 2), lax.rem(r, 2), y, z)

    def by_col(q):
        q = lax.rem(q + 32, 32)
        return (x, c, lax.div(q, NZ), lax.rem(q, NZ))

    near = [by_row(row + 1), by_row(row - 1), by_col(col + 1), by_col(col - 1)]
    valid = [row > 0, row < 7, col > 0, col < 31]
    reaches = [row < 7, row > 0, col < 31, col > 0]
    me_zc = z * 2 + c

    def zc_peer(k):
        t = lax.rem(me_zc + k, 16)
        return (x, lax.rem(t, 2), y, lax.div(t, 2))

    def y_peer(k):
        return (x, c, lax.rem(y + k, NY), z)

    def x_peer(k):
        return (lax.rem(x + k, NX), c, y, z)

    me_xy = x * NY + y

    def xy_peer(k):
        return (lax.rem(x + k // 4, NX), c, lax.rem(y + k % 4, NY), z)

    barrier = pltpu.get_barrier_semaphore()
    peers = near + [zc_peer(k) for k in range(1, 16)] + [xy_peer(k) for k in range(1, 16)]
    for peer in peers:
        pl.semaphore_signal(barrier, inc=1, device_id=peer, device_id_type=MESH)

    for i, (src, dst) in enumerate(
        ((sends0_h, sends0), (sends1_h, sends1), (agg1_h, agg1), (cols0_h, cols0), (agg0_h, agg0), (cols1_h, cols1))
    ):
        load(NB + 7 + i, src, dst)
    load(NB + 4, rhs.at[0, 0], rhs_v)
    load(NB + 5, diag0.at[0, 0], diag0_v)
    load(NB + 6, diag1.at[0, 0], diag1_v)
    load(NB + 2, pro1.at[0, 0], land_p1)
    for b in range(NB):
        load(b, blocks0.at[0, 0, b], land0.at[b])
    load(NB, pro0.at[0, 0], land_p0)
    load(NB + 1, blocks1.at[0, 0], land1)
    load(NB + 3, cinv, cin.at[c])
    sent, sent_near, due = [], [], {}

    def post(key, src, dst, ssem, rsem, peer, landing, landed):
        copy = pltpu.make_async_remote_copy(
            src_ref=src, dst_ref=dst, send_sem=ssem, recv_sem=rsem, device_id=peer, device_id_type=MESH
        )
        copy.start()
        sent.append(copy)
        due[key] = pltpu.make_async_remote_copy(
            src_ref=landing, dst_ref=landing, send_sem=ssem, recv_sem=landed, device_id=peer, device_id_type=MESH
        )

    def take(*key):
        due.pop(key).wait_recv()

    def post_near(key, src, dst, ssem, rsem, d):
        copy = pltpu.make_async_remote_copy(
            src_ref=src, dst_ref=dst, send_sem=ssem, recv_sem=rsem, device_id=near[d], device_id_type=MESH
        )
        pl.when(reaches[d])(copy.start)
        sent_near.append((d, copy))
        due[key] = (d, copy)

    def take_near(*key):
        d, copy = due.pop(key)
        pl.when(valid[d])(copy.wait_recv)


    def start_exchange(e, value, pick, pack, ghost, width, base):
        for d in range(4):
            for g in range(width):
                pack[e, d, g] = value[pick(d, g)]
        for d in range(4):
            post_near((base + e, d), pack.at[e, d], ghost.at[e, d], gs.at[base + e, d], gr.at[base + e, d], d)

    def own_part(value, ext, count):
        for b in range(count):
            hi, lo = halves(value[b])
            ext[b, 0:4] = hi
            ext[b, 4:8] = lo

    def end_exchange(e, ghost, ext, width, base, count):
        for d in range(4):
            take_near(base + e, d)
            for g in range(width):
                hi, lo = halves(jnp.where(valid[d], ghost[e, d, g], 0.0))
                ext[count + d * width + g, 0:4] = hi
                ext[count + d * width + g, 4:8] = lo

    def coupled(b, ext, cols, w):
        v = jnp.concatenate([ext[cols[0, 0, b, k]] for k in range(K)], axis=1).astype(BF16)
        return fold(dot(v, w[b], NN))

    def each(count, body):
        if unroll >= count:
            for b in range(count):
                body(b)
        else:
            def step(t, carry):
                for u in range(unroll):
                    body(t * unroll + u)
                return carry
            lax.fori_loop(0, count // unroll, step, 0)

    def sweep(right, diag, value, ext, cols, w, count):
        def body(b):
            d = diag[b]
            v = value[b]
            value[b] = v + OMEGA * (right[b] - (d * v + coupled(b, ext, cols, w))) / d
        each(count, body)

    def residual(right, diag, value, ext, cols, w, count, res):
        def body(b):
            res[b] = right[b] - (diag[b] * value[b] + coupled(b, ext, cols, w))
        each(count, body)

    class First:
        def __init__(self, ref, vector):
            self.ref, self.vector = ref, vector

        def __getitem__(self, b):
            return self.ref[pl.ds(b, 1), :] if self.vector else self.ref[b]

    f0, d0, d1 = rhs_v, First(diag0_v, True), First(diag1_v, True)

    def level0(e):
        start_exchange(e, x0, lambda d, g: sends0[0, 0, d, g], pack0, ghost0, G0, 0)

    def level0_end(e):
        own_part(x0, ext0, NB)
        end_exchange(e, ghost0, ext0, G0, 0, NB)

    def level1(e):
        start_exchange(e, x1, lambda d, g: sends1[0, 0, g, d], pack1, ghost1, G1, 4)

    def level1_end(e):
        own_part(x1, ext1, NB1)
        end_exchange(e, ghost1, ext1, G1, 4, NB1)

    for n in range(4, 13):
        loads.pop(NB + n).wait()
    for b in range(NB):
        x0[b] = OMEGA * f0[b] / d0[b]
    pl.semaphore_wait(barrier, len(peers))
    level0(0)

    loads.pop(NB + 2).wait()
    spot = lax.broadcasted_iota(jnp.int32, (4, 256), 1)
    rr = lax.broadcasted_iota(jnp.int32, (4, 256), 0)

    def rows_of(a):
        ax, ag, ay, ah = lax.div(a, 16), lax.rem(lax.div(a, 8), 2), lax.rem(lax.div(a, 2), 4), lax.rem(a, 2)
        base = (ax * 4 + ay) * 16 + ah * 4 + ag * 2
        return jnp.where(spot == base + lax.div(rr, 2) * 8 + lax.rem(rr, 2), 1.0, 0.0)

    for d in range(4):
        for g in range(G1):
            pp1[d, g] = land_p1[sends1[0, 0, g, d]]
            ps1[d, g] = rows_of(agg1[0, 0, sends1[0, 0, g, d]])
    for d in range(4):
        post_near(("pp", d), pp1.at[d], gp1.at[d], gs.at[8, d], gr.at[8, d], d)
        post_near(("ps", d), ps1.at[d], gsel.at[d], gs.at[9, d], gr.at[9, d], d)
    lanes = lax.broadcasted_iota(jnp.int32, (2, BS), 1)
    osend[0:2, :] = jnp.where(lanes == agg1[0, 0, 0], 1.0, 0.0)
    osend[2:4, :] = jnp.where(lanes == agg1[0, 0, 1], 1.0, 0.0)
    oz[me_zc] = osend[...]
    for k in (8, 7, 9, 6, 10, 5, 11, 4, 12, 3, 13, 2, 14, 1, 15):
        t = lax.rem(me_zc + k, 16)
        post(("oz", k), osend, oz.at[me_zc], ozs.at[k], ozr.at[me_zc], zc_peer(k), oz.at[t], ozr.at[t])

    eye = jnp.where(
        lax.broadcasted_iota(jnp.int32, (256, 256), 0) == lax.broadcasted_iota(jnp.int32, (256, 256), 1), 1.0, 0.0
    ).astype(BF16)

    def split0(b, carry):
        pltpu.make_async_copy(blocks0.at[0, 0, b], land0.at[b], lsem.at[b]).wait()
        for k in range(0, K, 2):
            w0[b, k * BS:(k + 2) * BS, :] = turned(eye, land0[b, k], land0[b, k + 1])
        return carry

    lax.fori_loop(0, NB, split0, 0)
    for b in range(NB):
        loads.pop(b)

    level0_end(0)
    sweep(f0, d0, x0, ext0, cols0, w0, NB)
    level0(1)
    own_part(x0, ext0, NB)

    loads.pop(NB).wait()
    for b in range(NB):
        hi, lo = split(land_p0[b])
        p0[b * BS:(b + 1) * BS, 0:BS] = hi
        p0[b * BS:(b + 1) * BS, BS:2 * BS] = lo
    loads.pop(NB + 3).wait()
    post(("cin",), cin.at[c], cin.at[c], cs, cr, (x, 1 - c, y, z), cin.at[1 - c], cr)
    for k in range(1, 16):
        take("oz", k)
    oy[y] = oz[...]
    for k in (2, 1, 3):
        t = lax.rem(y + k, NY)
        post(("oy", k), oz, oy.at[y], oys.at[k], oyr.at[y], y_peer(k), oy.at[t], oyr.at[t])

    end_exchange(1, ghost0, ext0, G0, 0, NB)
    residual(f0, d0, x0, ext0, cols0, w0, NB, r0)
    parts = [[], []]
    for b in range(NB):
        both = jnp.concatenate(halves(r0[b]), axis=0)
        for level in range(NB1):
            parts[level].append(jnp.where(agg0[0, 0, b] == level, both, 0.0))
    lhs = jnp.concatenate([jnp.concatenate(p, axis=1) for p in parts], axis=0).astype(BF16)
    low = dot(lhs, p0[...], NN)
    for level in range(NB1):
        b1[level] = fold(low[level * 8:level * 8 + 8])
        x1[level] = OMEGA * b1[level] / d1[level]
    level1(0)

    loads.pop(NB + 1).wait()
    for b in range(NB1):
        for k in range(0, K, 2):
            w1[b, k * BS:(k + 2) * BS, :] = turned(eye, land1[b, k], land1[b, k + 1])
    for b in range(NB1):
        hi, lo = split(land_p1[b])
        p1[b, :, 0:BS] = hi
        p1[b, :, BS:2 * BS] = lo
        sel[b * 4:b * 4 + 4, :] = rows_of(agg1[0, 0, b]).astype(BF16)
    for d in range(4):
        take_near("pp", d)
        take_near("ps", d)
        for g in range(G1):
            n = NB1 + d * G1 + g
            hi, lo = split(jnp.where(valid[d], gp1[d, g], 0.0))
            p1[n, :, 0:BS] = hi
            p1[n, :, BS:2 * BS] = lo
            sel[n * 4:n * 4 + 4, :] = jnp.where(valid[d], gsel[d, g], 0.0).astype(BF16)
    level1_end(0)
    sweep(b1, d1, x1, ext1, cols1, w1, NB1)
    level1(1)
    own_part(x1, ext1, NB1)

    for k in range(1, 4):
        take("oy", k)
    rows = []
    for q in range(NY):
        for t in range(8):
            rows.append(jnp.concatenate([oy[q, 2 * t], oy[q, 2 * t + 1]], axis=0))
    ot[...] = jnp.concatenate(rows, axis=0).T.astype(BF16)

    end_exchange(1, ghost1, ext1, G1, 4, NB1)
    for b in range(NB1):
        r1 = b1[b] - (d1[b] * x1[b] + coupled(b, ext1, cols1, w1))
        con = fold(dot(eight(r1), p1[b], NN))
        dsend[0, b * 2:b * 2 + 2, :] = con[0:2]
        dsend[1, b * 2:b * 2 + 2, :] = con[2:4]
    dz[me_zc] = dsend[c]
    for k in (8, 7, 9, 6, 10, 5, 11, 4, 12, 3, 13, 2, 14, 1, 15):
        peer = zc_peer(k)
        t = lax.rem(me_zc + k, 16)
        post(("dz", k), dsend.at[peer[1]], dz.at[me_zc], dzs.at[k], dzr.at[me_zc], peer, dz.at[t], dzr.at[t])
    take("cin")
    for k in range(1, 16):
        take("dz", k)
    dy[y] = dz[...]
    for k in (2, 1, 3):
        t = lax.rem(y + k, NY)
        post(("dy", k), dz, dy.at[y], dys.at[k], dyr.at[y], y_peer(k), dy.at[t], dyr.at[t])
    for k in range(1, 4):
        take("dy", k)
    rows = []
    for q in range(NY):
        for t in range(8):
            rows.append(jnp.concatenate([dy[q, 2 * t], dy[q, 2 * t + 1]], axis=0))
    got = jnp.concatenate(rows, axis=0)
    odd = lax.rem(lax.broadcasted_iota(jnp.int32, got.shape, 0), 2)
    ghi, glo = halves(got)
    rhs4 = jnp.concatenate(
        [jnp.where(odd == 0, ghi, 0.0), jnp.where(odd == 1, ghi, 0.0), jnp.where(odd == 0, glo, 0.0), jnp.where(odd == 1, glo, 0.0)],
        axis=1,
    ).astype(BF16)
    dense = dot(ot[...], rhs4, NN)
    xsend[...] = dense[0:64, 0:256] + dense[0:64, 256:512]
    for k in (2, 1, 3):
        t = lax.rem(x + k, NX)
        post(("x", k), xsend, xg.at[x], xs.at[k], xr.at[x], x_peer(k), xg.at[t], xr.at[t])
    total = xsend[...]
    for k in range(1, 4):
        t = lax.rem(x + k, NX)
        take("x", k)
        total = total + xg[t]
    crhs[0] = total[:, 0:BS]
    crhs[1] = total[:, BS:2 * BS]

    def mat(t, acc):
        acc = list(acc)
        vec = [crhs[r, pl.ds(t, 1), :] for r in range(2)]
        for g in range(2):
            for m in range(4):
                a = cin[g, m * 8:m * 8 + 8, pl.ds(pl.multiple_of(t * BS, BS), BS)]
                for r in range(2):
                    acc[(g * 2 + r) * 4 + m] = acc[(g * 2 + r) * 4 + m] + a * vec[r]
        return tuple(acc)

    acc = lax.fori_loop(0, 64, mat, tuple(jnp.zeros((8, BS), F32) for _ in range(16)), unroll=4)
    zl = lax.rem(z, 4)
    chunks = []
    for q in range(4):
        for part in halves(jnp.concatenate(acc[q * 4:q * 4 + 4], axis=0)):
            chunks.append(jnp.concatenate([jnp.where(zl == s, part, 0.0) for s in range(4)], axis=0))
    place = jnp.concatenate(chunks, axis=1).astype(BF16)
    lhs_row = lax.broadcasted_iota(jnp.int32, (8, 8 * BS), 0)
    lhs_col = lax.div(lax.broadcasted_iota(jnp.int32, (8, 8 * BS), 1), 2 * BS)
    ones = jnp.where(lhs_row == lhs_col, 1.0, 0.0).astype(BF16)
    ez[me_zc] = dot(ones, place, NT)[0:4]
    for k in (8, 7, 9, 6, 10, 5, 11, 4, 12, 3, 13, 2, 14, 1, 15):
        t = lax.rem(me_zc + k, 16)
        post(("ez", k), ez.at[me_zc], ez.at[me_zc], ezs.at[k], ezr.at[me_zc], zc_peer(k), ez.at[t], ezr.at[t])
    for k in range(1, 16):
        take("ez", k)
    for h in range(2):
        for core in range(2):
            n = [ez[(4 * h + q) * 2 + core] for q in range(4)]
            ef[me_xy, core * 2 + h] = (n[0] + n[1]) + (n[2] + n[3])
    for k in (10, 9, 11, 6, 14, 2, 8, 5, 7, 13, 15, 1, 3, 4, 12):
        t = xy_peer(k)
        n = t[0] * NY + t[2]
        post(("ef", k), ef.at[me_xy], ef.at[me_xy], efs.at[k], efr.at[me_xy], t, ef.at[n], efr.at[n])
    for k in range(1, 16):
        take("ef", k)
    every = jnp.concatenate(
        [jnp.concatenate([ef[n, 2 * m], ef[n, 2 * m + 1]], axis=0) for n in range(16) for m in range(2)], axis=0
    )
    both = dot(sel[...], jnp.concatenate(split(every), axis=1), NN)
    picked = both[:, 0:BS] + both[:, BS:2 * BS]
    for n in range(NB1 + 4 * G1):
        e8 = eight(picked[n * 4:n * 4 + 4])
        o = dot(jnp.concatenate([e8, e8], axis=1), p1[n], NT)
        o = o[0:4] + o[4:8]
        if n < NB1:
            x1[n] = x1[n] + o
        else:
            hi, lo = halves(ext1[n, 0:4] + ext1[n, 4:8] + o)
            ext1[n, 0:4] = hi
            ext1[n, 4:8] = lo
    own_part(x1, ext1, NB1)
    for e in (2, 3):
        if e == 3:
            level1(e)
            level1_end(e)
        sweep(b1, d1, x1, ext1, cols1, w1, NB1)

    for b in range(NB):
        e8 = eight(x1[agg0[0, 0, b]])
        o = dot(jnp.concatenate([e8, e8], axis=1), p0[b * BS:(b + 1) * BS, :], NT)
        x0[b] = x0[b] + (o[0:4] + o[4:8])
    for e in (2, 3):
        level0(e)
        level0_end(e)
        sweep(f0, d0, x0, ext0, cols0, w0, NB)
    for b in range(NB):
        out[0, 0, b] = x0[b]
    for copy in sent:
        copy.wait_send()
    for d, copy in sent_near:
        pl.when(reaches[d])(copy.wait_send)


def on_device(rhs, diag0, blocks0, cols0, sends0, pro0, agg0, diag1, blocks1, cols1, sends1, pro1, agg1, cinv, unroll=8):
    vmem = pl.BlockSpec(memory_space=pltpu.VMEM)
    hbm = pl.BlockSpec(memory_space=pl.ANY)
    V = pltpu.VMEM
    dma = pltpu.SemaphoreType.DMA
    S = pltpu.SMEM
    index = [cols0, sends0, agg0, cols1, sends1.transpose(0, 1, 3, 2), agg1]
    scratch = [
        *[S(a.shape, jnp.int32) for a in index],
        V((NB, R, BS), F32), V((NB, BS), F32), V((NB1, BS), F32),
        V((NB, K, BS, BS), F32), V((NB, BS, BS), F32), V((NB1, K, BS, BS), F32), V((NB1, BS, BS), F32), V((2, 32, 8192), F32),
        V((NB, K * BS, 2 * BS), BF16), V((NB * BS, 2 * BS), BF16), V((NB1, K * BS, 2 * BS), BF16), V((NB1 + 4 * G1, BS, 2 * BS), BF16), V((40, 256), BF16),
        V((4, G1, BS, BS), F32), V((4, G1, BS, BS), F32), V((4, G1, 4, 256), F32), V((4, G1, 4, 256), F32),
        V((NB + 4 * G0, 8, BS), F32), V((NB1 + 4 * G1, 8, BS), F32),
        V((NB, R, BS), F32), V((NB, R, BS), F32), V((NB1, R, BS), F32), V((NB1, R, BS), F32),
        V((4, 4, G0, R, BS), F32), V((4, 4, G0, R, BS), F32), V((4, 4, G1, R, BS), F32), V((4, 4, G1, R, BS), F32),
        V((4, BS), F32), V((16, 4, BS), F32), V((4, 16, 4, BS), F32), V((BS, 256), BF16),
        V((2, 4, BS), F32), V((16, 4, BS), F32), V((4, 16, 4, BS), F32),
        V((64, 256), F32), V((4, 64, 256), F32), V((2, 64, BS), F32),
        V((16, 4, BS), F32), V((16, 4, 4, BS), F32),
        dma((NB + 13,)), dma((10, 4)), dma((10, 4)),
        dma((16,)), dma((16,)), dma((4,)), dma((4,)),
        dma((16,)), dma((16,)), dma((4,)), dma((4,)),
        dma((4,)), dma((4,)), dma((16,)), dma((16,)), dma((16,)), dma((16,)),
        dma, dma,
    ]

    def body(*refs):
        kernel(*refs, unroll=unroll)

    return pl.pallas_call(
        body,
        out_shape=jax.ShapeDtypeStruct(rhs.shape, F32),
        in_specs=[hbm] * 14,
        out_specs=vmem,
        scratch_shapes=scratch,
        compiler_params=pltpu.CompilerParams(collective_id=0, has_side_effects=True, vmem_limit_bytes=60 * 1024 * 1024),
        name="vcycle",
    )(
        *index, rhs, diag0, diag1, blocks0, pro0, blocks1, pro1, cinv,
    )


def solution(mesh):
    finer = Mesh(mesh.devices.reshape(NX, NC, NY, NZ), ("x", "c", "y", "z"))
    ROW, COL = ("x", "c"), ("y", "z")
    ranks = (3, 2, 4, 2, 2, 3, 1, 2, 4, 2, 2, 3, 1)
    in_specs = tuple(P(ROW, COL, *([None] * n)) for n in ranks) + (P(ROW + COL, None),)
    return jax.shard_map(
        on_device, mesh=finer, in_specs=in_specs, out_specs=P(ROW, COL, None, None, None), check_vma=False
    )
```

```python
import jax
import jax.numpy as jnp
from jax import lax
from jax.experimental import pallas as pl
from jax.experimental.pallas import tpu as pltpu
from jax.sharding import Mesh
from jax.sharding import PartitionSpec as P

OMEGA = 0.3
NX, NC, NY, NZ = 4, 2, 4, 8
BS = 128
NB, NB1, K, G0, G1, R = 8, 2, 14, 4, 2, 4
F32, BF16 = jnp.float32, jnp.bfloat16
MESH = pl.DeviceIdType.MESH
NT = (((1,), (1,)), ((), ()))
NN = (((1,), (0,)), ((), ()))


def split(v):
    hi = v.astype(BF16)
    lo = (v - hi.astype(F32)).astype(BF16)
    return hi, lo


def turned(eye, left, right):
    both = [jnp.concatenate(pair, axis=1) for pair in zip(split(left), split(right))]
    return dot(eye, jnp.concatenate(both, axis=0), NT).astype(BF16)


def halves(v):
    hi = v.astype(BF16).astype(F32)
    return hi, v - hi


def eight(v):
    hi, lo = halves(v)
    return jnp.concatenate([hi, lo], axis=0).astype(BF16)


def fold(out):
    n = out.shape[1] // 2
    return (out[0:4, :n] + out[0:4, n:]) + (out[4:8, :n] + out[4:8, n:])


def dot(a, b, dims):
    return lax.dot_general(a, b, dims, preferred_element_type=F32)


def kernel(
    cols0_h, sends0_h, agg0_h, cols1_h, sends1_h, agg1_h,
    rhs, diag0, diag1, blocks0, pro0, blocks1, pro1, cinv,
    out,
    cols0, sends0, agg0, cols1, sends1, agg1,
    rhs_v, diag0_v, diag1_v,
    land0, land_p0, land1, land_p1, cin,
    w0, p0, w1, p1, sel, pp1, gp1, ps1, gsel,
    ext0, ext1, x0, r0, x1, b1, pack0, ghost0, pack1, ghost1,
    osend, oz, oy, ot, dsend, dz, dy, xsend, xg, crhs, ez, ef,
    heard, lsem, gs, gr, ozs, ozr, oys, oyr, dzs, dzr, dys, dyr, xs, xr, ezs, ezr, efs, efr, cs, cr,
    unroll,
):
    x, c, y, z = (lax.axis_index(a) for a in ("x", "c", "y", "z"))
    row = x * NC + c
    col = y * NZ + z
    loads = {}

    def load(i, src, dst):
        copy = pltpu.make_async_copy(src, dst, lsem.at[i])
        copy.start()
        loads[i] = copy

    def by_row(r):
        r = lax.rem(r + 8, 8)
        return (lax.div(r, 2), lax.rem(r, 2), y, z)

    def by_col(q):
        q = lax.rem(q + 32, 32)
        return (x, c, lax.div(q, NZ), lax.rem(q, NZ))

    near = [by_row(row + 1), by_row(row - 1), by_col(col + 1), by_col(col - 1)]
    valid = [row > 0, row < 7, col > 0, col < 31]
    reaches = [row < 7, row > 0, col < 31, col > 0]
    me_zc = z * 2 + c

    def zc_peer(k):
        t = lax.rem(me_zc + k, 16)
        return (x, lax.rem(t, 2), y, lax.div(t, 2))

    def y_peer(k):
        return (x, c, lax.rem(y + k, NY), z)

    def x_peer(k):
        return (lax.rem(x + k, NX), c, y, z)

    me_xy = x * NY + y

    def xy_peer(k):
        return (lax.rem(x + k // 4, NX), c, lax.rem(y + k % 4, NY), z)

    barrier = pltpu.get_barrier_semaphore()
    sides = [
        (x, c, y, lax.rem(z + 1, NZ)), (x, c, y, lax.rem(z + NZ - 1, NZ)), y_peer(1), y_peer(3), x_peer(1), x_peer(3),
    ]
    peers = near + sides + [(x, 1 - c, y, z)]
    for peer in peers:
        pl.semaphore_signal(barrier, inc=1, device_id=peer, device_id_type=MESH)

    for i, (src, dst) in enumerate(
        ((sends0_h, sends0), (sends1_h, sends1), (agg1_h, agg1), (cols0_h, cols0), (agg0_h, agg0), (cols1_h, cols1))
    ):
        load(NB + 7 + i, src, dst)
    load(NB + 4, rhs.at[0, 0], rhs_v)
    load(NB + 5, diag0.at[0, 0], diag0_v)
    load(NB + 6, diag1.at[0, 0], diag1_v)
    load(NB + 2, pro1.at[0, 0], land_p1)
    for b in range(NB):
        load(b, blocks0.at[0, 0, b], land0.at[b])
    load(NB, pro0.at[0, 0], land_p0)
    load(NB + 1, blocks1.at[0, 0], land1)
    load(NB + 3, cinv, cin.at[c])
    sent, sent_near, due = [], [], {}

    def post(key, src, dst, ssem, rsem, peer, landing, landed):
        copy = pltpu.make_async_remote_copy(
            src_ref=src, dst_ref=dst, send_sem=ssem, recv_sem=rsem, device_id=peer, device_id_type=MESH
        )
        copy.start()
        sent.append(copy)
        due[key] = pltpu.make_async_remote_copy(
            src_ref=landing, dst_ref=landing, send_sem=ssem, recv_sem=landed, device_id=peer, device_id_type=MESH
        )

    def take(*key):
        due.pop(key).wait_recv()

    def post_near(key, src, dst, ssem, rsem, d):
        copy = pltpu.make_async_remote_copy(
            src_ref=src, dst_ref=dst, send_sem=ssem, recv_sem=rsem, device_id=near[d], device_id_type=MESH
        )
        pl.when(reaches[d])(copy.start)
        sent_near.append((d, copy))
        due[key] = (d, copy)

    def take_near(*key):
        d, copy = due.pop(key)
        pl.when(valid[d])(copy.wait_recv)

    def tell(n):
        for side in sides:
            pl.semaphore_signal(heard.at[n], inc=1, device_id=side, device_id_type=MESH)

    def hear(n):
        pl.semaphore_wait(heard.at[n], len(sides))


    def start_exchange(e, value, pick, pack, ghost, width, base):
        for d in range(4):
            for g in range(width):
                pack[e, d, g] = value[pick(d, g)]
        for d in range(4):
            post_near((base + e, d), pack.at[e, d], ghost.at[e, d], gs.at[base + e, d], gr.at[base + e, d], d)

    def own_part(value, ext, count):
        for b in range(count):
            hi, lo = halves(value[b])
            ext[b, 0:4] = hi
            ext[b, 4:8] = lo

    def end_exchange(e, ghost, ext, width, base, count):
        for d in range(4):
            take_near(base + e, d)
            for g in range(width):
                hi, lo = halves(jnp.where(valid[d], ghost[e, d, g], 0.0))
                ext[count + d * width + g, 0:4] = hi
                ext[count + d * width + g, 4:8] = lo

    def coupled(b, ext, cols, w):
        v = jnp.concatenate([ext[cols[0, 0, b, k]] for k in range(K)], axis=1).astype(BF16)
        return fold(dot(v, w[b], NN))

    def each(count, body):
        if unroll >= count:
            for b in range(count):
                body(b)
        else:
            def step(t, carry):
                for u in range(unroll):
                    body(t * unroll + u)
                return carry
            lax.fori_loop(0, count // unroll, step, 0)

    def sweep(right, diag, value, ext, cols, w, count):
        def body(b):
            d = diag[b]
            v = value[b]
            value[b] = v + OMEGA * (right[b] - (d * v + coupled(b, ext, cols, w))) / d
        each(count, body)

    def residual(right, diag, value, ext, cols, w, count, res):
        def body(b):
            res[b] = right[b] - (diag[b] * value[b] + coupled(b, ext, cols, w))
        each(count, body)

    class First:
        def __init__(self, ref, vector):
            self.ref, self.vector = ref, vector

        def __getitem__(self, b):
            return self.ref[pl.ds(b, 1), :] if self.vector else self.ref[b]

    f0, d0, d1 = rhs_v, First(diag0_v, True), First(diag1_v, True)

    def level0(e):
        start_exchange(e, x0, lambda d, g: sends0[0, 0, d, g], pack0, ghost0, G0, 0)

    def level0_end(e):
        own_part(x0, ext0, NB)
        end_exchange(e, ghost0, ext0, G0, 0, NB)

    def level1(e):
        start_exchange(e, x1, lambda d, g: sends1[0, 0, g, d], pack1, ghost1, G1, 4)

    def level1_end(e):
        own_part(x1, ext1, NB1)
        end_exchange(e, ghost1, ext1, G1, 4, NB1)

    for n in range(4, 13):
        loads.pop(NB + n).wait()
    for b in range(NB):
        x0[b] = OMEGA * f0[b] / d0[b]
    pl.semaphore_wait(barrier, len(peers))
    level0(0)

    loads.pop(NB + 2).wait()
    spot = lax.broadcasted_iota(jnp.int32, (4, 256), 1)
    rr = lax.broadcasted_iota(jnp.int32, (4, 256), 0)

    def rows_of(a):
        ax, ag, ay, ah = lax.div(a, 16), lax.rem(lax.div(a, 8), 2), lax.rem(lax.div(a, 2), 4), lax.rem(a, 2)
        base = (ax * 4 + ay) * 16 + ah * 4 + ag * 2
        return jnp.where(spot == base + lax.div(rr, 2) * 8 + lax.rem(rr, 2), 1.0, 0.0)

    for d in range(4):
        for g in range(G1):
            pp1[d, g] = land_p1[sends1[0, 0, g, d]]
            ps1[d, g] = rows_of(agg1[0, 0, sends1[0, 0, g, d]])
    for d in range(4):
        post_near(("pp", d), pp1.at[d], gp1.at[d], gs.at[8, d], gr.at[8, d], d)
        post_near(("ps", d), ps1.at[d], gsel.at[d], gs.at[9, d], gr.at[9, d], d)
    lanes = lax.broadcasted_iota(jnp.int32, (2, BS), 1)
    osend[0:2, :] = jnp.where(lanes == agg1[0, 0, 0], 1.0, 0.0)
    osend[2:4, :] = jnp.where(lanes == agg1[0, 0, 1], 1.0, 0.0)
    oz[me_zc] = osend[...]
    tell(0)

    eye = jnp.where(
        lax.broadcasted_iota(jnp.int32, (256, 256), 0) == lax.broadcasted_iota(jnp.int32, (256, 256), 1), 1.0, 0.0
    ).astype(BF16)

    def split0(b, carry):
        pltpu.make_async_copy(blocks0.at[0, 0, b], land0.at[b], lsem.at[b]).wait()
        for k in range(0, K, 2):
            w0[b, k * BS:(k + 2) * BS, :] = turned(eye, land0[b, k], land0[b, k + 1])
        return carry

    lax.fori_loop(0, NB, split0, 0)
    for b in range(NB):
        loads.pop(b)

    hear(0)
    tell(1)
    level0_end(0)
    sweep(f0, d0, x0, ext0, cols0, w0, NB)
    level0(1)
    own_part(x0, ext0, NB)

    loads.pop(NB).wait()
    for b in range(NB):
        hi, lo = split(land_p0[b])
        p0[b * BS:(b + 1) * BS, 0:BS] = hi
        p0[b * BS:(b + 1) * BS, BS:2 * BS] = lo
    loads.pop(NB + 3).wait()
    post(("cin",), cin.at[c], cin.at[c], cs, cr, (x, 1 - c, y, z), cin.at[1 - c], cr)
    hear(1)
    tell(2)

    end_exchange(1, ghost0, ext0, G0, 0, NB)
    hear(2)
    tell(3)
    residual(f0, d0, x0, ext0, cols0, w0, NB, r0)
    parts = [[], []]
    for b in range(NB):
        both = jnp.concatenate(halves(r0[b]), axis=0)
        for level in range(NB1):
            parts[level].append(jnp.where(agg0[0, 0, b] == level, both, 0.0))
    lhs = jnp.concatenate([jnp.concatenate(p, axis=1) for p in parts], axis=0).astype(BF16)
    low = dot(lhs, p0[...], NN)
    for level in range(NB1):
        b1[level] = fold(low[level * 8:level * 8 + 8])
        x1[level] = OMEGA * b1[level] / d1[level]
    level1(0)
    hear(3)
    for k in (8, 7, 9, 6, 10, 5, 11, 4, 12, 3, 13, 2, 14, 1, 15):
        t = lax.rem(me_zc + k, 16)
        post(("oz", k), osend, oz.at[me_zc], ozs.at[k], ozr.at[me_zc], zc_peer(k), oz.at[t], ozr.at[t])

    loads.pop(NB + 1).wait()
    for b in range(NB1):
        for k in range(0, K, 2):
            w1[b, k * BS:(k + 2) * BS, :] = turned(eye, land1[b, k], land1[b, k + 1])
    for b in range(NB1):
        hi, lo = split(land_p1[b])
        p1[b, :, 0:BS] = hi
        p1[b, :, BS:2 * BS] = lo
        sel[b * 4:b * 4 + 4, :] = rows_of(agg1[0, 0, b]).astype(BF16)
    for d in range(4):
        take_near("pp", d)
        take_near("ps", d)
        for g in range(G1):
            n = NB1 + d * G1 + g
            hi, lo = split(jnp.where(valid[d], gp1[d, g], 0.0))
            p1[n, :, 0:BS] = hi
            p1[n, :, BS:2 * BS] = lo
            sel[n * 4:n * 4 + 4, :] = jnp.where(valid[d], gsel[d, g], 0.0).astype(BF16)
    level1_end(0)
    sweep(b1, d1, x1, ext1, cols1, w1, NB1)
    level1(1)
    own_part(x1, ext1, NB1)

    for k in range(1, 16):
        take("oz", k)
    oy[y] = oz[...]
    for k in (2, 1, 3):
        t = lax.rem(y + k, NY)
        post(("oy", k), oz, oy.at[y], oys.at[k], oyr.at[y], y_peer(k), oy.at[t], oyr.at[t])

    end_exchange(1, ghost1, ext1, G1, 4, NB1)
    for b in range(NB1):
        r1 = b1[b] - (d1[b] * x1[b] + coupled(b, ext1, cols1, w1))
        con = fold(dot(eight(r1), p1[b], NN))
        dsend[0, b * 2:b * 2 + 2, :] = con[0:2]
        dsend[1, b * 2:b * 2 + 2, :] = con[2:4]
    dz[me_zc] = dsend[c]
    for k in (8, 7, 9, 6, 10, 5, 11, 4, 12, 3, 13, 2, 14, 1, 15):
        peer = zc_peer(k)
        t = lax.rem(me_zc + k, 16)
        post(("dz", k), dsend.at[peer[1]], dz.at[me_zc], dzs.at[k], dzr.at[me_zc], peer, dz.at[t], dzr.at[t])
    for k in range(1, 4):
        take("oy", k)
    rows = []
    for q in range(NY):
        for t in range(8):
            rows.append(jnp.concatenate([oy[q, 2 * t], oy[q, 2 * t + 1]], axis=0))
    ot[...] = jnp.concatenate(rows, axis=0).T.astype(BF16)
    take("cin")
    for k in range(1, 16):
        take("dz", k)
    dy[y] = dz[...]
    for k in (2, 1, 3):
        t = lax.rem(y + k, NY)
        post(("dy", k), dz, dy.at[y], dys.at[k], dyr.at[y], y_peer(k), dy.at[t], dyr.at[t])
    for k in range(1, 4):
        take("dy", k)
    rows = []
    for q in range(NY):
        for t in range(8):
            rows.append(jnp.concatenate([dy[q, 2 * t], dy[q, 2 * t + 1]], axis=0))
    got = jnp.concatenate(rows, axis=0)
    odd = lax.rem(lax.broadcasted_iota(jnp.int32, got.shape, 0), 2)
    ghi, glo = halves(got)
    rhs4 = jnp.concatenate(
        [jnp.where(odd == 0, ghi, 0.0), jnp.where(odd == 1, ghi, 0.0), jnp.where(odd == 0, glo, 0.0), jnp.where(odd == 1, glo, 0.0)],
        axis=1,
    ).astype(BF16)
    dense = dot(ot[...], rhs4, NN)
    xsend[...] = dense[0:64, 0:256] + dense[0:64, 256:512]
    for k in (2, 1, 3):
        t = lax.rem(x + k, NX)
        post(("x", k), xsend, xg.at[x], xs.at[k], xr.at[x], x_peer(k), xg.at[t], xr.at[t])
    total = xsend[...]
    for k in range(1, 4):
        t = lax.rem(x + k, NX)
        take("x", k)
        total = total + xg[t]
    crhs[0] = total[:, 0:BS]
    crhs[1] = total[:, BS:2 * BS]

    def mat(t, acc):
        acc = list(acc)
        vec = [crhs[r, pl.ds(t, 1), :] for r in range(2)]
        for g in range(2):
            for m in range(4):
                a = cin[g, m * 8:m * 8 + 8, pl.ds(pl.multiple_of(t * BS, BS), BS)]
                for r in range(2):
                    acc[(g * 2 + r) * 4 + m] = acc[(g * 2 + r) * 4 + m] + a * vec[r]
        return tuple(acc)

    acc = lax.fori_loop(0, 64, mat, tuple(jnp.zeros((8, BS), F32) for _ in range(16)), unroll=4)
    zl = lax.rem(z, 4)
    chunks = []
    for q in range(4):
        for part in halves(jnp.concatenate(acc[q * 4:q * 4 + 4], axis=0)):
            chunks.append(jnp.concatenate([jnp.where(zl == s, part, 0.0) for s in range(4)], axis=0))
    place = jnp.concatenate(chunks, axis=1).astype(BF16)
    lhs_row = lax.broadcasted_iota(jnp.int32, (8, 8 * BS), 0)
    lhs_col = lax.div(lax.broadcasted_iota(jnp.int32, (8, 8 * BS), 1), 2 * BS)
    ones = jnp.where(lhs_row == lhs_col, 1.0, 0.0).astype(BF16)
    ez[me_zc] = dot(ones, place, NT)[0:4]
    for k in (8, 7, 9, 6, 10, 5, 11, 4, 12, 3, 13, 2, 14, 1, 15):
        t = lax.rem(me_zc + k, 16)
        post(("ez", k), ez.at[me_zc], ez.at[me_zc], ezs.at[k], ezr.at[me_zc], zc_peer(k), ez.at[t], ezr.at[t])
    for k in range(1, 16):
        take("ez", k)
    for h in range(2):
        for core in range(2):
            n = [ez[(4 * h + q) * 2 + core] for q in range(4)]
            ef[me_xy, core * 2 + h] = (n[0] + n[1]) + (n[2] + n[3])
    for k in (10, 9, 11, 6, 14, 2, 8, 5, 7, 13, 15, 1, 3, 4, 12):
        t = xy_peer(k)
        n = t[0] * NY + t[2]
        post(("ef", k), ef.at[me_xy], ef.at[me_xy], efs.at[k], efr.at[me_xy], t, ef.at[n], efr.at[n])
    for k in range(1, 16):
        take("ef", k)
    every = jnp.concatenate(
        [jnp.concatenate([ef[n, 2 * m], ef[n, 2 * m + 1]], axis=0) for n in range(16) for m in range(2)], axis=0
    )
    both = dot(sel[...], jnp.concatenate(split(every), axis=1), NN)
    picked = both[:, 0:BS] + both[:, BS:2 * BS]
    for n in range(NB1 + 4 * G1):
        e8 = eight(picked[n * 4:n * 4 + 4])
        o = dot(jnp.concatenate([e8, e8], axis=1), p1[n], NT)
        o = o[0:4] + o[4:8]
        if n < NB1:
            x1[n] = x1[n] + o
        else:
            hi, lo = halves(ext1[n, 0:4] + ext1[n, 4:8] + o)
            ext1[n, 0:4] = hi
            ext1[n, 4:8] = lo
    own_part(x1, ext1, NB1)
    for e in (2, 3):
        if e == 3:
            level1(e)
            level1_end(e)
        sweep(b1, d1, x1, ext1, cols1, w1, NB1)

    for b in range(NB):
        e8 = eight(x1[agg0[0, 0, b]])
        o = dot(jnp.concatenate([e8, e8], axis=1), p0[b * BS:(b + 1) * BS, :], NT)
        x0[b] = x0[b] + (o[0:4] + o[4:8])
    for e in (2, 3):
        level0(e)
        level0_end(e)
        sweep(f0, d0, x0, ext0, cols0, w0, NB)
    for b in range(NB):
        out[0, 0, b] = x0[b]
    for copy in sent:
        copy.wait_send()
    for d, copy in sent_near:
        pl.when(reaches[d])(copy.wait_send)


def on_device(rhs, diag0, blocks0, cols0, sends0, pro0, agg0, diag1, blocks1, cols1, sends1, pro1, agg1, cinv, unroll=8):
    vmem = pl.BlockSpec(memory_space=pltpu.VMEM)
    hbm = pl.BlockSpec(memory_space=pl.ANY)
    V = pltpu.VMEM
    dma = pltpu.SemaphoreType.DMA
    S = pltpu.SMEM
    index = [cols0, sends0, agg0, cols1, sends1.transpose(0, 1, 3, 2), agg1]
    scratch = [
        *[S(a.shape, jnp.int32) for a in index],
        V((NB, R, BS), F32), V((NB, BS), F32), V((NB1, BS), F32),
        V((NB, K, BS, BS), F32), V((NB, BS, BS), F32), V((NB1, K, BS, BS), F32), V((NB1, BS, BS), F32), V((2, 32, 8192), F32),
        V((NB, K * BS, 2 * BS), BF16), V((NB * BS, 2 * BS), BF16), V((NB1, K * BS, 2 * BS), BF16), V((NB1 + 4 * G1, BS, 2 * BS), BF16), V((40, 256), BF16),
        V((4, G1, BS, BS), F32), V((4, G1, BS, BS), F32), V((4, G1, 4, 256), F32), V((4, G1, 4, 256), F32),
        V((NB + 4 * G0, 8, BS), F32), V((NB1 + 4 * G1, 8, BS), F32),
        V((NB, R, BS), F32), V((NB, R, BS), F32), V((NB1, R, BS), F32), V((NB1, R, BS), F32),
        V((4, 4, G0, R, BS), F32), V((4, 4, G0, R, BS), F32), V((4, 4, G1, R, BS), F32), V((4, 4, G1, R, BS), F32),
        V((4, BS), F32), V((16, 4, BS), F32), V((4, 16, 4, BS), F32), V((BS, 256), BF16),
        V((2, 4, BS), F32), V((16, 4, BS), F32), V((4, 16, 4, BS), F32),
        V((64, 256), F32), V((4, 64, 256), F32), V((2, 64, BS), F32),
        V((16, 4, BS), F32), V((16, 4, 4, BS), F32),
        pltpu.SemaphoreType.REGULAR((4,)), dma((NB + 13,)), dma((10, 4)), dma((10, 4)),
        dma((16,)), dma((16,)), dma((4,)), dma((4,)),
        dma((16,)), dma((16,)), dma((4,)), dma((4,)),
        dma((4,)), dma((4,)), dma((16,)), dma((16,)), dma((16,)), dma((16,)),
        dma, dma,
    ]

    def body(*refs):
        kernel(*refs, unroll=unroll)

    return pl.pallas_call(
        body,
        out_shape=jax.ShapeDtypeStruct(rhs.shape, F32),
        in_specs=[hbm] * 14,
        out_specs=vmem,
        scratch_shapes=scratch,
        compiler_params=pltpu.CompilerParams(collective_id=0, has_side_effects=True, vmem_limit_bytes=60 * 1024 * 1024),
        name="vcycle",
    )(
        *index, rhs, diag0, diag1, blocks0, pro0, blocks1, pro1, cinv,
    )


def solution(mesh):
    finer = Mesh(mesh.devices.reshape(NX, NC, NY, NZ), ("x", "c", "y", "z"))
    ROW, COL = ("x", "c"), ("y", "z")
    ranks = (3, 2, 4, 2, 2, 3, 1, 2, 4, 2, 2, 3, 1)
    in_specs = tuple(P(ROW, COL, *([None] * n)) for n in ranks) + (P(ROW + COL, None),)
    return jax.shard_map(
        on_device, mesh=finer, in_specs=in_specs, out_specs=P(ROW, COL, None, None, None), check_vma=False
    )
```

```python
import jax
import jax.numpy as jnp
from jax import lax
from jax.experimental import pallas as pl
from jax.experimental.pallas import tpu as pltpu
from jax.sharding import Mesh
from jax.sharding import PartitionSpec as P

OMEGA = 0.3
NX, NC, NY, NZ = 4, 2, 4, 8
BS = 128
NB, NB1, K, G0, G1, R = 8, 2, 14, 4, 2, 4
F32, BF16 = jnp.float32, jnp.bfloat16
MESH = pl.DeviceIdType.MESH
NT = (((1,), (1,)), ((), ()))
NN = (((1,), (0,)), ((), ()))


def split(v):
    hi = v.astype(BF16)
    lo = (v - hi.astype(F32)).astype(BF16)
    return hi, lo


def turned(eye, left, right):
    both = [jnp.concatenate(pair, axis=1) for pair in zip(split(left), split(right))]
    return dot(eye, jnp.concatenate(both, axis=0), NT).astype(BF16)


def halves(v):
    hi = v.astype(BF16).astype(F32)
    return hi, v - hi


def eight(v):
    hi, lo = halves(v)
    return jnp.concatenate([hi, lo], axis=0).astype(BF16)


def fold(out):
    n = out.shape[1] // 2
    return (out[0:4, :n] + out[0:4, n:]) + (out[4:8, :n] + out[4:8, n:])


def dot(a, b, dims):
    return lax.dot_general(a, b, dims, preferred_element_type=F32)


def kernel(
    cols0_h, sends0_h, agg0_h, cols1_h, sends1_h, agg1_h,
    rhs, diag0, diag1, blocks0, pro0, blocks1, pro1, cinv,
    out,
    cols0, sends0, agg0, cols1, sends1, agg1,
    rhs_v, diag0_v, diag1_v,
    land0, land_p0, land1, land_p1, cin,
    w0, p0, w1, p1, sel, pp1, gp1, ps1, gsel,
    ext0, ext1, x0, r0, x1, b1, pack0, ghost0, pack1, ghost1,
    osend, oz, oy, ot, dsend, dz, dy, xsend, xg, crhs, ez, ef,
    heard, lsem, gs, gr, ozs, ozr, oys, oyr, dzs, dzr, dys, dyr, xs, xr, ezs, ezr, efs, efr, cs, cr,
    unroll,
):
    x, c, y, z = (lax.axis_index(a) for a in ("x", "c", "y", "z"))
    row = x * NC + c
    col = y * NZ + z
    loads = {}

    def load(i, src, dst):
        copy = pltpu.make_async_copy(src, dst, lsem.at[i])
        copy.start()
        loads[i] = copy

    def by_row(r):
        r = lax.rem(r + 8, 8)
        return (lax.div(r, 2), lax.rem(r, 2), y, z)

    def by_col(q):
        q = lax.rem(q + 32, 32)
        return (x, c, lax.div(q, NZ), lax.rem(q, NZ))

    near = [by_row(row + 1), by_row(row - 1), by_col(col + 1), by_col(col - 1)]
    valid = [row > 0, row < 7, col > 0, col < 31]
    reaches = [row < 7, row > 0, col < 31, col > 0]
    me_zc = z * 2 + c

    def zc_peer(k):
        t = lax.rem(me_zc + k, 16)
        return (x, lax.rem(t, 2), y, lax.div(t, 2))

    def y_peer(k):
        return (x, c, lax.rem(y + k, NY), z)

    def x_peer(k):
        return (lax.rem(x + k, NX), c, y, z)

    me_xy = x * NY + y

    def xy_peer(k):
        return (lax.rem(x + k // 4, NX), c, lax.rem(y + k % 4, NY), z)

    barrier = pltpu.get_barrier_semaphore()
    sides = [
        (x, c, y, lax.rem(z + 1, NZ)), (x, c, y, lax.rem(z + NZ - 1, NZ)), y_peer(1), y_peer(3), x_peer(1), x_peer(3),
    ]
    peers = sides + [(x, 1 - c, y, z)]
    for peer in peers:
        pl.semaphore_signal(barrier, inc=1, device_id=peer, device_id_type=MESH)

    def greet(d):
        pl.semaphore_signal(barrier, inc=1, device_id=near[d], device_id_type=MESH)

    for d in range(4):
        pl.when(reaches[d])(lambda d=d: greet(d))

    for i, (src, dst) in enumerate(
        ((sends0_h, sends0), (sends1_h, sends1), (agg1_h, agg1), (cols0_h, cols0), (agg0_h, agg0), (cols1_h, cols1))
    ):
        load(NB + 7 + i, src, dst)
    load(NB + 4, rhs.at[0, 0], rhs_v)
    load(NB + 5, diag0.at[0, 0], diag0_v)
    load(NB + 6, diag1.at[0, 0], diag1_v)
    load(NB + 2, pro1.at[0, 0], land_p1)
    for b in range(NB):
        load(b, blocks0.at[0, 0, b], land0.at[b])
    load(NB, pro0.at[0, 0], land_p0)
    load(NB + 1, blocks1.at[0, 0], land1)
    load(NB + 3, cinv, cin.at[c])
    sent, sent_near, due = [], [], {}

    def post(key, src, dst, ssem, rsem, peer, landing, landed):
        copy = pltpu.make_async_remote_copy(
            src_ref=src, dst_ref=dst, send_sem=ssem, recv_sem=rsem, device_id=peer, device_id_type=MESH
        )
        copy.start()
        sent.append(copy)
        due[key] = pltpu.make_async_remote_copy(
            src_ref=landing, dst_ref=landing, send_sem=ssem, recv_sem=landed, device_id=peer, device_id_type=MESH
        )

    def take(*key):
        due.pop(key).wait_recv()

    def post_near(key, src, dst, ssem, rsem, d):
        copy = pltpu.make_async_remote_copy(
            src_ref=src, dst_ref=dst, send_sem=ssem, recv_sem=rsem, device_id=near[d], device_id_type=MESH
        )
        pl.when(reaches[d])(copy.start)
        sent_near.append((d, copy))
        due[key] = (d, copy)

    def take_near(*key):
        d, copy = due.pop(key)
        pl.when(valid[d])(copy.wait_recv)

    def tell(n):
        for side in sides:
            pl.semaphore_signal(heard.at[n], inc=1, device_id=side, device_id_type=MESH)

    def hear(n):
        pl.semaphore_wait(heard.at[n], len(sides))


    def start_exchange(e, value, pick, pack, ghost, width, base):
        for d in (2, 3, 0, 1):
            for g in range(width):
                pack[e, d, g] = value[pick(d, g)]
            post_near((base + e, d), pack.at[e, d], ghost.at[e, d], gs.at[base + e, d], gr.at[base + e, d], d)

    def own_part(value, ext, count):
        for b in range(count):
            hi, lo = halves(value[b])
            ext[b, 0:4] = hi
            ext[b, 4:8] = lo

    def end_exchange(e, ghost, ext, width, base, count):
        for d in range(4):
            take_near(base + e, d)
            for g in range(width):
                hi, lo = halves(jnp.where(valid[d], ghost[e, d, g], 0.0))
                ext[count + d * width + g, 0:4] = hi
                ext[count + d * width + g, 4:8] = lo

    def coupled(b, ext, cols, w):
        v = jnp.concatenate([ext[cols[0, 0, b, k]] for k in range(K)], axis=1).astype(BF16)
        return fold(dot(v, w[b], NN))

    def each(count, body):
        if unroll >= count:
            for b in range(count):
                body(b)
        else:
            def step(t, carry):
                for u in range(unroll):
                    body(t * unroll + u)
                return carry
            lax.fori_loop(0, count // unroll, step, 0)

    def sweep(right, diag, value, ext, cols, w, count):
        def body(b):
            d = diag[b]
            v = value[b]
            value[b] = v + OMEGA * (right[b] - (d * v + coupled(b, ext, cols, w))) / d
        each(count, body)

    def residual(right, diag, value, ext, cols, w, count, res):
        def body(b):
            res[b] = right[b] - (diag[b] * value[b] + coupled(b, ext, cols, w))
        each(count, body)

    class First:
        def __init__(self, ref, vector):
            self.ref, self.vector = ref, vector

        def __getitem__(self, b):
            return self.ref[pl.ds(b, 1), :] if self.vector else self.ref[b]

    f0, d0, d1 = rhs_v, First(diag0_v, True), First(diag1_v, True)

    def level0(e):
        start_exchange(e, x0, lambda d, g: sends0[0, 0, d, g], pack0, ghost0, G0, 0)

    def level0_end(e):
        own_part(x0, ext0, NB)
        end_exchange(e, ghost0, ext0, G0, 0, NB)

    def level1(e):
        start_exchange(e, x1, lambda d, g: sends1[0, 0, g, d], pack1, ghost1, G1, 4)

    def level1_end(e):
        own_part(x1, ext1, NB1)
        end_exchange(e, ghost1, ext1, G1, 4, NB1)

    for n in range(4, 13):
        loads.pop(NB + n).wait()
    for b in range(NB):
        x0[b] = OMEGA * f0[b] / d0[b]
    pl.semaphore_wait(barrier, len(peers) + sum(jnp.where(v, 1, 0) for v in valid))
    level0(0)

    loads.pop(NB + 2).wait()
    spot = lax.broadcasted_iota(jnp.int32, (4, 256), 1)
    rr = lax.broadcasted_iota(jnp.int32, (4, 256), 0)

    def rows_of(a):
        ax, ag, ay, ah = lax.div(a, 16), lax.rem(lax.div(a, 8), 2), lax.rem(lax.div(a, 2), 4), lax.rem(a, 2)
        base = (ax * 4 + ay) * 16 + ah * 4 + ag * 2
        return jnp.where(spot == base + lax.div(rr, 2) * 8 + lax.rem(rr, 2), 1.0, 0.0)

    for d in range(4):
        for g in range(G1):
            pp1[d, g] = land_p1[sends1[0, 0, g, d]]
            ps1[d, g] = rows_of(agg1[0, 0, sends1[0, 0, g, d]])
    for d in range(4):
        post_near(("pp", d), pp1.at[d], gp1.at[d], gs.at[8, d], gr.at[8, d], d)
        post_near(("ps", d), ps1.at[d], gsel.at[d], gs.at[9, d], gr.at[9, d], d)
    lanes = lax.broadcasted_iota(jnp.int32, (2, BS), 1)
    osend[0:2, :] = jnp.where(lanes == agg1[0, 0, 0], 1.0, 0.0)
    osend[2:4, :] = jnp.where(lanes == agg1[0, 0, 1], 1.0, 0.0)
    oz[me_zc] = osend[...]
    tell(0)

    eye = jnp.where(
        lax.broadcasted_iota(jnp.int32, (256, 256), 0) == lax.broadcasted_iota(jnp.int32, (256, 256), 1), 1.0, 0.0
    ).astype(BF16)

    def split0(b, carry):
        pltpu.make_async_copy(blocks0.at[0, 0, b], land0.at[b], lsem.at[b]).wait()
        for k in range(0, K, 2):
            w0[b, k * BS:(k + 2) * BS, :] = turned(eye, land0[b, k], land0[b, k + 1])
        return carry

    lax.fori_loop(0, NB, split0, 0)
    for b in range(NB):
        loads.pop(b)

    hear(0)
    tell(1)
    level0_end(0)
    sweep(f0, d0, x0, ext0, cols0, w0, NB)
    level0(1)
    own_part(x0, ext0, NB)

    loads.pop(NB).wait()
    for b in range(NB):
        hi, lo = split(land_p0[b])
        p0[b * BS:(b + 1) * BS, 0:BS] = hi
        p0[b * BS:(b + 1) * BS, BS:2 * BS] = lo
    loads.pop(NB + 3).wait()
    post(("cin",), cin.at[c], cin.at[c], cs, cr, (x, 1 - c, y, z), cin.at[1 - c], cr)
    hear(1)
    tell(2)

    end_exchange(1, ghost0, ext0, G0, 0, NB)
    hear(2)
    tell(3)
    residual(f0, d0, x0, ext0, cols0, w0, NB, r0)
    parts = [[], []]
    for b in range(NB):
        both = jnp.concatenate(halves(r0[b]), axis=0)
        for level in range(NB1):
            parts[level].append(jnp.where(agg0[0, 0, b] == level, both, 0.0))
    lhs = jnp.concatenate([jnp.concatenate(p, axis=1) for p in parts], axis=0).astype(BF16)
    low = dot(lhs, p0[...], NN)
    for level in range(NB1):
        b1[level] = fold(low[level * 8:level * 8 + 8])
        x1[level] = OMEGA * b1[level] / d1[level]
    level1(0)
    hear(3)
    for k in (8, 7, 9, 6, 10, 5, 11, 4, 12, 3, 13, 2, 14, 1, 15):
        t = lax.rem(me_zc + k, 16)
        post(("oz", k), osend, oz.at[me_zc], ozs.at[k], ozr.at[me_zc], zc_peer(k), oz.at[t], ozr.at[t])

    loads.pop(NB + 1).wait()
    for b in range(NB1):
        for k in range(0, K, 2):
            w1[b, k * BS:(k + 2) * BS, :] = turned(eye, land1[b, k], land1[b, k + 1])
    for b in range(NB1):
        hi, lo = split(land_p1[b])
        p1[b, :, 0:BS] = hi
        p1[b, :, BS:2 * BS] = lo
        sel[b * 4:b * 4 + 4, :] = rows_of(agg1[0, 0, b]).astype(BF16)
    for d in range(4):
        take_near("pp", d)
        take_near("ps", d)
        for g in range(G1):
            n = NB1 + d * G1 + g
            hi, lo = split(jnp.where(valid[d], gp1[d, g], 0.0))
            p1[n, :, 0:BS] = hi
            p1[n, :, BS:2 * BS] = lo
            sel[n * 4:n * 4 + 4, :] = jnp.where(valid[d], gsel[d, g], 0.0).astype(BF16)
    level1_end(0)
    sweep(b1, d1, x1, ext1, cols1, w1, NB1)
    level1(1)
    own_part(x1, ext1, NB1)

    for k in range(1, 16):
        take("oz", k)
    oy[y] = oz[...]
    for k in (2, 1, 3):
        t = lax.rem(y + k, NY)
        post(("oy", k), oz, oy.at[y], oys.at[k], oyr.at[y], y_peer(k), oy.at[t], oyr.at[t])

    end_exchange(1, ghost1, ext1, G1, 4, NB1)
    for b in range(NB1):
        r1 = b1[b] - (d1[b] * x1[b] + coupled(b, ext1, cols1, w1))
        con = fold(dot(eight(r1), p1[b], NN))
        dsend[0, b * 2:b * 2 + 2, :] = con[0:2]
        dsend[1, b * 2:b * 2 + 2, :] = con[2:4]
    dz[me_zc] = dsend[c]
    for k in (8, 7, 9, 6, 10, 5, 11, 4, 12, 3, 13, 2, 14, 1, 15):
        peer = zc_peer(k)
        t = lax.rem(me_zc + k, 16)
        post(("dz", k), dsend.at[peer[1]], dz.at[me_zc], dzs.at[k], dzr.at[me_zc], peer, dz.at[t], dzr.at[t])
    for k in range(1, 4):
        take("oy", k)
    rows = []
    for q in range(NY):
        for t in range(8):
            rows.append(jnp.concatenate([oy[q, 2 * t], oy[q, 2 * t + 1]], axis=0))
    ot[...] = jnp.concatenate(rows, axis=0).T.astype(BF16)
    take("cin")
    for k in range(1, 16):
        take("dz", k)
    dy[y] = dz[...]
    for k in (2, 1, 3):
        t = lax.rem(y + k, NY)
        post(("dy", k), dz, dy.at[y], dys.at[k], dyr.at[y], y_peer(k), dy.at[t], dyr.at[t])
    for k in range(1, 4):
        take("dy", k)
    rows = []
    for q in range(NY):
        for t in range(8):
            rows.append(jnp.concatenate([dy[q, 2 * t], dy[q, 2 * t + 1]], axis=0))
    got = jnp.concatenate(rows, axis=0)
    odd = lax.rem(lax.broadcasted_iota(jnp.int32, got.shape, 0), 2)
    ghi, glo = halves(got)
    rhs4 = jnp.concatenate(
        [jnp.where(odd == 0, ghi, 0.0), jnp.where(odd == 1, ghi, 0.0), jnp.where(odd == 0, glo, 0.0), jnp.where(odd == 1, glo, 0.0)],
        axis=1,
    ).astype(BF16)
    dense = dot(ot[...], rhs4, NN)
    xsend[...] = dense[0:64, 0:256] + dense[0:64, 256:512]
    for k in (2, 1, 3):
        t = lax.rem(x + k, NX)
        post(("x", k), xsend, xg.at[x], xs.at[k], xr.at[x], x_peer(k), xg.at[t], xr.at[t])
    total = xsend[...]
    for k in range(1, 4):
        t = lax.rem(x + k, NX)
        take("x", k)
        total = total + xg[t]
    crhs[0] = total[:, 0:BS]
    crhs[1] = total[:, BS:2 * BS]

    def mat(t, acc):
        acc = list(acc)
        vec = [crhs[r, pl.ds(t, 1), :] for r in range(2)]
        for g in range(2):
            for m in range(4):
                a = cin[g, m * 8:m * 8 + 8, pl.ds(pl.multiple_of(t * BS, BS), BS)]
                for r in range(2):
                    acc[(g * 2 + r) * 4 + m] = acc[(g * 2 + r) * 4 + m] + a * vec[r]
        return tuple(acc)

    acc = lax.fori_loop(0, 64, mat, tuple(jnp.zeros((8, BS), F32) for _ in range(16)), unroll=16)
    zl = lax.rem(z, 4)
    chunks = []
    for q in range(4):
        for part in halves(jnp.concatenate(acc[q * 4:q * 4 + 4], axis=0)):
            chunks.append(jnp.concatenate([jnp.where(zl == s, part, 0.0) for s in range(4)], axis=0))
    place = jnp.concatenate(chunks, axis=1).astype(BF16)
    lhs_row = lax.broadcasted_iota(jnp.int32, (8, 8 * BS), 0)
    lhs_col = lax.div(lax.broadcasted_iota(jnp.int32, (8, 8 * BS), 1), 2 * BS)
    ones = jnp.where(lhs_row == lhs_col, 1.0, 0.0).astype(BF16)
    ez[me_zc] = dot(ones, place, NT)[0:4]
    for k in (8, 7, 9, 6, 10, 5, 11, 4, 12, 3, 13, 2, 14, 1, 15):
        t = lax.rem(me_zc + k, 16)
        post(("ez", k), ez.at[me_zc], ez.at[me_zc], ezs.at[k], ezr.at[me_zc], zc_peer(k), ez.at[t], ezr.at[t])
    for k in range(1, 16):
        take("ez", k)
    for h in range(2):
        for core in range(2):
            n = [ez[(4 * h + q) * 2 + core] for q in range(4)]
            ef[me_xy, core * 2 + h] = (n[0] + n[1]) + (n[2] + n[3])
    for k in (10, 9, 11, 6, 14, 2, 8, 5, 7, 13, 15, 1, 3, 4, 12):
        t = xy_peer(k)
        n = t[0] * NY + t[2]
        post(("ef", k), ef.at[me_xy], ef.at[me_xy], efs.at[k], efr.at[me_xy], t, ef.at[n], efr.at[n])
    for k in range(1, 16):
        take("ef", k)
    every = jnp.concatenate(
        [jnp.concatenate([ef[n, 2 * m], ef[n, 2 * m + 1]], axis=0) for n in range(16) for m in range(2)], axis=0
    )
    both = dot(sel[...], jnp.concatenate(split(every), axis=1), NN)
    picked = both[:, 0:BS] + both[:, BS:2 * BS]
    for n in range(NB1 + 4 * G1):
        e8 = eight(picked[n * 4:n * 4 + 4])
        o = dot(jnp.concatenate([e8, e8], axis=1), p1[n], NT)
        o = o[0:4] + o[4:8]
        if n < NB1:
            x1[n] = x1[n] + o
        else:
            hi, lo = halves(ext1[n, 0:4] + ext1[n, 4:8] + o)
            ext1[n, 0:4] = hi
            ext1[n, 4:8] = lo
    own_part(x1, ext1, NB1)
    for e in (2, 3):
        if e == 3:
            level1(e)
            level1_end(e)
        sweep(b1, d1, x1, ext1, cols1, w1, NB1)

    for b in range(NB):
        e8 = eight(x1[agg0[0, 0, b]])
        o = dot(jnp.concatenate([e8, e8], axis=1), p0[b * BS:(b + 1) * BS, :], NT)
        x0[b] = x0[b] + (o[0:4] + o[4:8])
    for e in (2, 3):
        level0(e)
        level0_end(e)
        sweep(f0, d0, x0, ext0, cols0, w0, NB)
    for b in range(NB):
        out[0, 0, b] = x0[b]
    for copy in sent:
        copy.wait_send()
    for d, copy in sent_near:
        pl.when(reaches[d])(copy.wait_send)


def on_device(rhs, diag0, blocks0, cols0, sends0, pro0, agg0, diag1, blocks1, cols1, sends1, pro1, agg1, cinv, unroll=8):
    vmem = pl.BlockSpec(memory_space=pltpu.VMEM)
    hbm = pl.BlockSpec(memory_space=pl.ANY)
    V = pltpu.VMEM
    dma = pltpu.SemaphoreType.DMA
    S = pltpu.SMEM
    index = [cols0, sends0, agg0, cols1, sends1.transpose(0, 1, 3, 2), agg1]
    scratch = [
        *[S(a.shape, jnp.int32) for a in index],
        V((NB, R, BS), F32), V((NB, BS), F32), V((NB1, BS), F32),
        V((NB, K, BS, BS), F32), V((NB, BS, BS), F32), V((NB1, K, BS, BS), F32), V((NB1, BS, BS), F32), V((2, 32, 8192), F32),
        V((NB, K * BS, 2 * BS), BF16), V((NB * BS, 2 * BS), BF16), V((NB1, K * BS, 2 * BS), BF16), V((NB1 + 4 * G1, BS, 2 * BS), BF16), V((40, 256), BF16),
        V((4, G1, BS, BS), F32), V((4, G1, BS, BS), F32), V((4, G1, 4, 256), F32), V((4, G1, 4, 256), F32),
        V((NB + 4 * G0, 8, BS), F32), V((NB1 + 4 * G1, 8, BS), F32),
        V((NB, R, BS), F32), V((NB, R, BS), F32), V((NB1, R, BS), F32), V((NB1, R, BS), F32),
        V((4, 4, G0, R, BS), F32), V((4, 4, G0, R, BS), F32), V((4, 4, G1, R, BS), F32), V((4, 4, G1, R, BS), F32),
        V((4, BS), F32), V((16, 4, BS), F32), V((4, 16, 4, BS), F32), V((BS, 256), BF16),
        V((2, 4, BS), F32), V((16, 4, BS), F32), V((4, 16, 4, BS), F32),
        V((64, 256), F32), V((4, 64, 256), F32), V((2, 64, BS), F32),
        V((16, 4, BS), F32), V((16, 4, 4, BS), F32),
        pltpu.SemaphoreType.REGULAR((4,)), dma((NB + 13,)), dma((10, 4)), dma((10, 4)),
        dma((16,)), dma((16,)), dma((4,)), dma((4,)),
        dma((16,)), dma((16,)), dma((4,)), dma((4,)),
        dma((4,)), dma((4,)), dma((16,)), dma((16,)), dma((16,)), dma((16,)),
        dma, dma,
    ]

    def body(*refs):
        kernel(*refs, unroll=unroll)

    return pl.pallas_call(
        body,
        out_shape=jax.ShapeDtypeStruct(rhs.shape, F32),
        in_specs=[hbm] * 14,
        out_specs=vmem,
        scratch_shapes=scratch,
        compiler_params=pltpu.CompilerParams(collective_id=0, has_side_effects=True, vmem_limit_bytes=60 * 1024 * 1024),
        name="vcycle",
    )(
        *index, rhs, diag0, diag1, blocks0, pro0, blocks1, pro1, cinv,
    )


def solution(mesh):
    finer = Mesh(mesh.devices.reshape(NX, NC, NY, NZ), ("x", "c", "y", "z"))
    ROW, COL = ("x", "c"), ("y", "z")
    ranks = (3, 2, 4, 2, 2, 3, 1, 2, 4, 2, 2, 3, 1)
    in_specs = tuple(P(ROW, COL, *([None] * n)) for n in ranks) + (P(ROW + COL, None),)
    return jax.shard_map(
        on_device, mesh=finer, in_specs=in_specs, out_specs=P(ROW, COL, None, None, None), check_vma=False
    )
```
